512 devices in a mesh: head: 8 (over y, core), seq: 64 (over x, z).
Axes of the slice: x: 4, y: 4, z: 16, core: 2. Of those that a mesh axis runs over, the one named last changes fastest.
Arguments:
- query_vectors: bfloat16 [8192, 4096], P('seq', 'head'), may hold values from -1000 to 1000
- key_vectors: bfloat16 [8192, 4096], P('seq', 'head'), may hold values from -1000 to 1000
- value_vectors: bfloat16 [8192, 4096], P('seq', 'head'), may hold values from -6 to 6
- cluster: int32 [32, 8192], P('head', 'seq'), may hold values from 0 to 127, as said below
- centroids: float32 [32, 128, 128], P('head'), may hold values from -1.25 to 1.25
- upstream: bfloat16 [8192, 4096], P('seq', 'head'), may hold values from -6 to 6
Outputs:
- attended: bfloat16 [8192, 4096], P('seq', 'head')
- grad_queries: bfloat16 [8192, 4096], P('seq', 'head')
- grad_keys: bfloat16 [8192, 4096], P('seq', 'head')
- grad_values: bfloat16 [8192, 4096], P('seq', 'head')
- new_centroids: float32 [32, 128, 128], P('head')
The draws below stay inside these ranges and needn't reach their ends.
Inputs may be any that keep to these rules, and one draw needn't show every extreme that they name: In every head each cluster holds exactly 64 tokens. Of the 128 tokens of one index of seq at most 2 fall into one cluster of a head, and every cluster of every head receives exactly 2 from some index of seq. In each head the clusters fall into pairs whose counts from one index of seq add up to 2.
All inputs are finite; a program needn't handle non-finite values.
Results may differ from the reference program's by a relative error of at most 0.015.
Values may be sent and summed in bfloat16 or wider, within the bound.
A program may use at most 64 MiB of HBM per device.

```python
import jax
import jax.numpy as jnp
from jax import lax

HD = 128
TOK_DEV = 128
HEADS = 32
CLUSTERS = 128
TOKENS = 8192
WIDTH = 4096
CSIZE = 64
N_SEQ = 64


def route_table(key):
    base = TOK_DEV // CLUSTERS
    half = CLUSTERS // 2

    def one_head(head_key):
        splits = jax.random.split(head_key, 5)
        spread = jax.random.randint(splits[0], (N_SEQ // 2,), 0, base + 1)
        spread = spread.at[0].set(base)
        offsets = jax.random.permutation(splits[1], jnp.concatenate([spread, -spread]))
        shifts = jax.random.randint(splits[2], (half,), 0, N_SEQ)
        devices = jnp.arange(N_SEQ, dtype=jnp.int32)[:, None]
        swing = offsets[(devices + shifts[None, :]) % N_SEQ]
        pairing = jax.random.permutation(splits[3], CLUSTERS)
        counts = jnp.zeros((N_SEQ, CLUSTERS), jnp.int32)
        counts = counts.at[:, pairing[:half]].set(base + swing)
        counts = counts.at[:, pairing[half:]].set(base - swing)

        def one_device(row, device_key):
            labels = jnp.repeat(jnp.arange(CLUSTERS, dtype=jnp.int32), row, total_repeat_length=TOK_DEV)
            return jax.random.permutation(device_key, labels)
        device_keys = jax.random.split(splits[4], N_SEQ)
        rows = jax.vmap(one_device)(counts, device_keys)
        return rows.reshape(N_SEQ * TOK_DEV)
    return jax.vmap(one_head)(jax.random.split(key, HEADS)).astype(jnp.int32)


def feature_pair(key):
    parts = jax.random.split(key, 4)
    width = HEADS * HD
    head_place = (jnp.arange(width) // HD).astype(jnp.float32)
    column = 10.0 ** ((head_place + 0.5) / HEADS)
    query_rows = 10.0 ** jax.random.uniform(parts[0], (TOKENS, 1), minval=0.0, maxval=1.0)
    key_rows = 10.0 ** jax.random.uniform(parts[1], (TOKENS, 1), minval=0.0, maxval=1.0)
    query_base = jnp.clip(jax.random.normal(parts[2], (TOKENS, width)), -6.0, 6.0) * column[None, :] * query_rows
    key_base = jnp.clip(jax.random.normal(parts[3], (TOKENS, width)), -6.0, 6.0) * column[None, :] * key_rows
    return (query_base, key_base)


def draw_query_vectors(key, part):
    return feature_pair(key)[0].astype(jnp.bfloat16)


def draw_key_vectors(key, part):
    return feature_pair(key)[1].astype(jnp.bfloat16)


def draw_cluster(key, part):
    return route_table(jax.random.fold_in(key, 11))


def shard_levels(rng, dims, cuts, low, largest):
    loudness, own = 1.0, jax.random.fold_in(rng, 6)
    for axis_at, blocks in cuts:
        heights = jnp.exp(jax.random.uniform(jax.random.fold_in(own, axis_at), (blocks,), jnp.float32, low / len(cuts), largest / len(cuts)))
        loudness = loudness * jnp.repeat(heights, dims[axis_at] // blocks).reshape([-1 if axis == axis_at else 1 for axis in range(len(dims))])
    return loudness


def noise(key, shape, deviation, reach, cuts=(), kind=jnp.bfloat16):
    entries = deviation * jax.random.normal(key, shape, jnp.float32)
    if cuts:
        entries = entries * shard_levels(key, shape, cuts, -0.22, 0.18)
    return jnp.clip(entries, -reach, reach).astype(kind)


def setup_inputs(seed: int = 0) -> dict:
    streams_of = jax.random.split(jax.random.key(seed), 7)
    return {
        "query_vectors": draw_query_vectors(jax.random.fold_in(streams_of[6], 71), 0),
        "key_vectors": draw_key_vectors(jax.random.fold_in(streams_of[6], 71), 0),
        "value_vectors": noise(streams_of[2], (TOKENS, WIDTH), 1.0, 6.0, ((0, 64), (1, 8))),
        "cluster": draw_cluster(jax.random.fold_in(streams_of[6], 71), 0),
        "centroids": noise(streams_of[4], (HEADS, CLUSTERS, HD), 0.09, 1.25, ((0, 8),), jnp.float32),
        "upstream": noise(streams_of[5], (TOKENS, WIDTH), 1.0, 6.0, ((0, 64), (1, 8))),
    }


MASKED = -1e+30
EPSILON = 1e-06
RETAIN = 0.9

def attend_cluster(query_rows, key_rows, value_rows, upstream_rows):
    factor = HD ** (-0.5)
    places = jnp.arange(query_rows.shape[1], dtype=jnp.int32)
    allowed = (places[None, :] <= places[:, None])[None, :, :]
    query_wide = query_rows.astype(jnp.float32)
    key_wide = key_rows.astype(jnp.float32)
    value_wide = value_rows.astype(jnp.float32)
    upstream_wide = upstream_rows.astype(jnp.float32)
    scores = jnp.einsum('gsd,gtd->gst', query_wide, key_wide) * factor
    scores = jnp.where(allowed, scores, MASKED)
    row_max = lax.optimization_barrier(jnp.max(scores, axis=2, keepdims=True))
    raised = jnp.exp(scores - row_max)
    weights = raised / lax.optimization_barrier(jnp.sum(raised, axis=2, keepdims=True))
    weights_low = weights.astype(jnp.bfloat16)
    attended = jnp.einsum('gst,gtd->gsd', weights_low.astype(jnp.float32), value_wide).astype(jnp.bfloat16)
    row_dot = lax.optimization_barrier(jnp.sum(upstream_wide * attended.astype(jnp.float32), axis=2))
    grad_weights = jnp.einsum('gsd,gtd->gst', upstream_wide, value_wide)
    grad_scores = (weights * (grad_weights - row_dot[:, :, None]) * factor).astype(jnp.bfloat16)
    grad_scores_wide = grad_scores.astype(jnp.float32)
    grad_query = jnp.einsum('gst,gtd->gsd', grad_scores_wide, key_wide).astype(jnp.bfloat16)
    grad_key = jnp.einsum('gst,gsd->gtd', grad_scores_wide, query_wide).astype(jnp.bfloat16)
    grad_value = jnp.einsum('gst,gsd->gtd', weights_low.astype(jnp.float32), upstream_wide).astype(jnp.bfloat16)
    unit_keys = key_wide * lax.rsqrt(lax.optimization_barrier(jnp.sum(key_wide * key_wide, axis=2, keepdims=True)) + EPSILON)
    key_sums = lax.optimization_barrier(jnp.sum(unit_keys, axis=1))
    return (attended, grad_query, grad_key, grad_value, key_sums)

def reference(query_vectors, key_vectors, value_vectors, cluster, centroids, upstream):
    query_wide = query_vectors.astype(jnp.float32)
    key_wide = key_vectors.astype(jnp.float32)
    query_scale = lax.rsqrt(lax.optimization_barrier(jnp.sum(query_wide * query_wide, axis=1)) / WIDTH + EPSILON)
    key_scale = lax.rsqrt(lax.optimization_barrier(jnp.sum(key_wide * key_wide, axis=1)) / WIDTH + EPSILON)
    query_norm = query_wide * query_scale[:, None]
    key_norm = key_wide * key_scale[:, None]
    query_low = query_norm.astype(jnp.bfloat16)
    key_low = key_norm.astype(jnp.bfloat16)
    sorting = jnp.argsort(cluster * TOKENS + jnp.arange(TOKENS, dtype=jnp.int32)[None, :], axis=1).astype(jnp.int32)
    query_heads = query_low.reshape(TOKENS, HEADS, HD)
    key_heads = key_low.reshape(TOKENS, HEADS, HD)
    value_heads = value_vectors.reshape(TOKENS, HEADS, HD)
    upstream_heads = upstream.reshape(TOKENS, HEADS, HD)

    def per_head(inputs):
        members, head = inputs

        def pick(source):
            return source[members, head].reshape(CLUSTERS, CSIZE, HD)
        outputs = attend_cluster(pick(query_heads), pick(key_heads), pick(value_heads), pick(upstream_heads))

        def place(result):
            return jnp.zeros((TOKENS, HD), result.dtype).at[members].set(result.reshape(TOKENS, HD))
        return (place(outputs[0]), place(outputs[1]), place(outputs[2]), place(outputs[3]), outputs[4])
    results = lax.map(per_head, (sorting, jnp.arange(HEADS, dtype=jnp.int32)))

    def joined(stacked):
        return jnp.transpose(stacked, (1, 0, 2)).reshape(TOKENS, WIDTH)
    attended = joined(results[0])
    grad_query_low = joined(results[1])
    grad_key_low = joined(results[2])
    grad_values = joined(results[3])
    key_sums = results[4]
    query_inner = lax.optimization_barrier(jnp.sum(grad_query_low.astype(jnp.float32) * query_norm, axis=1))
    key_inner = lax.optimization_barrier(jnp.sum(grad_key_low.astype(jnp.float32) * key_norm, axis=1))
    grad_queries = (query_scale[:, None] * (grad_query_low.astype(jnp.float32) - query_norm * (query_inner / WIDTH)[:, None])).astype(jnp.bfloat16)
    grad_keys = (key_scale[:, None] * (grad_key_low.astype(jnp.float32) - key_norm * (key_inner / WIDTH)[:, None])).astype(jnp.bfloat16)
    blended = RETAIN * centroids + (1.0 - RETAIN) * key_sums
    new_centroids = blended * lax.rsqrt(lax.optimization_barrier(jnp.sum(blended * blended, axis=2, keepdims=True)) + EPSILON)
    return (attended, grad_queries, grad_keys, grad_values, new_centroids)
```

```python
import functools

import jax
import jax.numpy as jnp
from jax import lax
from jax.experimental import pallas as pl
from jax.experimental.pallas import tpu as pltpu
from jax.sharding import PartitionSpec as P

MASKED = -1e30
EPSILON = 1e-06
RETAIN = 0.9
MESH = pl.DeviceIdType.MESH
F32 = jnp.float32
BF16 = jnp.bfloat16

HD = 128
NS = 64
NX, NZ = 4, 16
NH = 8
HL = 4
T = 128
C = 128
WIDTH = 4096
ROWS = NS * 8


def iota(shape, dim):
    return lax.broadcasted_iota(jnp.int32, shape, dim)


def nt(a, b):
    return lax.dot_general(a, b, (((1,), (1,)), ((), ())), preferred_element_type=F32)


def tn(a, b):
    return lax.dot_general(a, b, (((0,), (0,)), ((), ())), preferred_element_type=F32)


def nn(a, b):
    return lax.dot_general(a, b, (((1,), (0,)), ((), ())), preferred_element_type=F32)


def to_row(column, eye):
    return jnp.sum(eye * column, axis=0, keepdims=True)


def to_col(row, eye):
    return jnp.sum(eye * row, axis=1, keepdims=True)


def peer_of(i, me):
    x, z = me // NZ, me % NZ
    e, j = i // NZ, i % NZ
    far = NZ // 2 - (j + 1) // 2
    dz = far * (2 * (j % 2) - 1) + NZ
    dx = NX - 1 - e
    return ((x + dx) % NX) * NZ + (z + dz) % NZ


def kernel(
    q_hbm, k_hbm, v_hbm, u_hbm, cl_hbm, cen_hbm,
    att_o, gq_o, gk_o, gv_o, cen_o,
    q_s, k_s, v_s, u_s, cl_s, cen_s,
    xs, qn_s, kn_s, gql_s, gkl_s, perm, permt, oht,
    sq_send, sq_recv, in_send, in_recv, cnt_send, cnt_recv, cen_send, cen_recv,
    f_send, f_recv, b_send, b_recv,
    load_sem, sq_ss, sq_rs, in_ss, in_rs, cnt_ss, cnt_rs, cen_ss, cen_rs,
    f_ss, f_rs, b_ss, b_rs,
):
    me = lax.axis_index("seq")
    hme = lax.axis_index("head")

    loads = [
        pltpu.make_async_copy(src, dst, load_sem.at[n])
        for n, (src, dst) in enumerate(
            ((cl_hbm, cl_s), (q_hbm, q_s), (k_hbm, k_s), (v_hbm, v_s), (u_hbm, u_s), (cen_hbm, cen_s))
        )
    ]
    for load in loads:
        load.start()

    barrier = pltpu.get_barrier_semaphore()

    def greet(i, carry):
        pl.semaphore_signal(barrier, 1, device_id=(hme, peer_of(i, me)), device_id_type=MESH)
        return carry

    lax.fori_loop(0, NS - 1, greet, 0)

    def greet_head(i, carry):
        pl.semaphore_signal(barrier, 1, device_id=((hme + 1 + i) % NH, me), device_id_type=MESH)
        return carry

    lax.fori_loop(0, NH - 1, greet_head, 0)

    def send_all(src_at, dst, ss, rs):
        def step(i, carry):
            p = peer_of(i, me)
            pltpu.make_async_remote_copy(
                src_ref=src_at(p), dst_ref=dst.at[me], send_sem=ss, recv_sem=rs,
                device_id=(hme, p), device_id_type=MESH,
            ).start()
            return carry

        lax.fori_loop(0, NS - 1, step, 0)

    def send_heads(src, dst, ss, rs):
        def step(i, carry):
            pltpu.make_async_remote_copy(
                src_ref=src, dst_ref=dst.at[hme], send_sem=ss, recv_sem=rs,
                device_id=((hme + 1 + i) % NH, me), device_id_type=MESH,
            ).start()
            return carry

        lax.fori_loop(0, NH - 1, step, 0)

    def wait_blocks(buf, n, sem):
        part = buf.at[pl.ds(0, n)]
        pltpu.make_async_copy(part, part, sem).wait()

    ic = iota((T, T), 0)
    il = iota((T, T), 1)
    eye = (ic == il).astype(F32)
    before = (ic < il).astype(F32)
    after = (ic > il).astype(F32)

    loads[0].wait()
    member, cnt_col, earlier, cnt_rows = [], [], [], []
    for h in range(HL):
        m = (ic == cl_s[h : h + 1, :]).astype(F32)
        member.append(m)
        mb = m.astype(BF16)
        n = jnp.sum(m, axis=1, keepdims=True)
        cnt_col.append(n)
        cnt_rows.append(to_row(n, eye))
        earlier.append(jnp.sum(tn(mb, mb) * before, axis=0, keepdims=True))
    cnt_own = jnp.concatenate(cnt_rows + [jnp.zeros((8 - HL, C), F32)], axis=0).astype(BF16)
    cnt_send[...] = cnt_own
    cnt_recv[me] = cnt_own

    loads[1].wait()
    loads[2].wait()
    qf = q_s[...].astype(F32)
    q_row = to_row(jnp.sum(qf * qf, axis=1, keepdims=True), eye)
    kf = k_s[...].astype(F32)
    k_row = to_row(jnp.sum(kf * kf, axis=1, keepdims=True), eye)
    sq_own = jnp.concatenate([q_row, k_row, jnp.zeros((6, T), F32)], axis=0)
    sq_send[...] = sq_own
    sq_recv[hme] = sq_own

    big_r = iota((ROWS, ROWS), 0)
    big_l = iota((ROWS, ROWS), 1)
    perm[...] = (big_r == ((big_l // 2) % 4) * T + (big_l // 8) * 2 + big_l % 2).astype(F32).astype(BF16)
    permt[...] = (big_l == ((big_r // 2) % 4) * T + (big_r // 8) * 2 + big_r % 2).astype(F32).astype(BF16)

    loads[3].wait()
    loads[4].wait()
    for h in range(HL):
        xs[h, 2 * T : 3 * T, :] = v_s[:, h * HD : (h + 1) * HD]
        xs[h, 3 * T : 4 * T, :] = u_s[:, h * HD : (h + 1) * HD]
    loads[5].wait()

    pl.semaphore_wait(barrier, NS - 1 + NH - 1)
    send_heads(sq_send, sq_recv, sq_ss, sq_rs)
    send_all(lambda p: cnt_send, cnt_recv, cnt_ss, cnt_rs)

    wait_blocks(sq_recv, NH - 1, sq_rs)
    squares = jnp.sum(sq_recv[...], axis=0)
    scales = lax.rsqrt(squares * (1.0 / WIDTH) + EPSILON)
    q_scale = to_col(scales[0:1, :], eye)
    k_scale = to_col(scales[1:2, :], eye)
    q_norm = q_s[...].astype(F32) * q_scale
    k_norm = k_s[...].astype(F32) * k_scale
    qn_s[...] = q_norm
    kn_s[...] = k_norm
    q_low = q_norm.astype(BF16)
    k_low = k_norm.astype(BF16)
    for h in range(HL):
        xs[h, 0:T, :] = q_low[:, h * HD : (h + 1) * HD]
        xs[h, T : 2 * T, :] = k_low[:, h * HD : (h + 1) * HD]

    wait_blocks(cnt_recv, NS - 1, cnt_rs)
    table = cnt_recv[...].astype(F32).reshape(ROWS, C).astype(BF16)
    slot = (iota((T, 1), 0) % 2).astype(F32)
    label_col, label_row, pick_lead, pick_other, renewed_at, place_col = [], [], [], [], [], []
    mine = me.astype(F32)
    for h in range(HL):
        spread = (iota((T, ROWS), 1) == (iota((T, ROWS), 0) // 2) * 8 + h).astype(F32).astype(BF16)
        counts = nn(spread, table)
        swing = counts - 1.0
        sb = swing.astype(BF16)
        gram = tn(sb, sb)
        n_row = jnp.sum(swing * swing, axis=0, keepdims=True)
        n_sum = n_row + to_col(n_row, eye)
        opposite = (n_sum + 2.0 * gram == 0.0).astype(F32)
        same = (n_sum - 2.0 * gram == 0.0).astype(F32)
        rank_row = jnp.sum(same * before, axis=0, keepdims=True)
        rank_col = jnp.sum(same * after, axis=1, keepdims=True)
        partner = jnp.where(rank_row == rank_col, opposite, 0.0)
        other_row = jnp.sum(partner * before, axis=0, keepdims=True)
        other_col = jnp.sum(partner * after, axis=1, keepdims=True)
        lead_rank_row = jnp.sum((1.0 - other_col) * before, axis=0, keepdims=True)
        lead_rank_col = jnp.sum((1.0 - other_row) * after, axis=1, keepdims=True)
        partner_rank_col = jnp.sum(partner * lead_rank_row, axis=1, keepdims=True)
        owner_col = jnp.where(other_col > 0.0, partner_rank_col, lead_rank_col)
        base = 8.0 * owner_col + other_col * (2.0 - cnt_col[h])
        place = jnp.sum(member[h] * base, axis=0, keepdims=True) + earlier[h]
        place_col.append(to_col(place, eye))
        target = jnp.concatenate([place + 2.0 * a for a in range(4)], axis=1).astype(jnp.int32)
        onehot = (big_r == target).astype(F32).astype(BF16)
        packed = nn(onehot, xs[h])
        f_send[h] = packed.reshape(NS, 8, HD).astype(BF16)
        f_recv[h, me] = f_send[h, me]
        send_all(lambda p: f_send.at[h, p], f_recv.at[h], f_ss.at[h], f_rs.at[h])
        lead_mine_row = jnp.where((other_row == 0.0) & (lead_rank_row == mine), 1.0, 0.0)
        lead_count = jnp.sum(counts * lead_mine_row, axis=1, keepdims=True)
        label = (slot < lead_count).astype(F32)
        label_col.append(label)
        label_row.append(to_row(label, eye))
        pick_lead.append(jnp.where((other_col == 0.0) & (owner_col == mine), 1.0, 0.0))
        pick_other.append(jnp.where((other_col > 0.0) & (owner_col == mine), 1.0, 0.0))
        renewed_at.append((owner_col * 8.0 + (2.0 * h) + other_col).astype(jnp.int32))

    for h in range(HL):
        for a in range(4):
            oht[h, a * T : (a + 1) * T, :] = (
                (iota((T, ROWS), 1) == (place_col[h] + 2.0 * a).astype(jnp.int32)).astype(F32).astype(BF16)
            )

    factor = HD ** (-0.5)
    causal = il <= ic
    renewed_rows = []
    for h in range(HL):
        wait_blocks(f_recv.at[h], NS - 1, f_rs.at[h])
        received = f_recv[h].astype(F32).reshape(ROWS, HD).astype(BF16)
        rows = nn(perm[...], received)
        k_wide = rows[T : 2 * T]
        u_wide = rows[3 * T : 4 * T]
        low = rows.astype(BF16)
        qr, kr, vr, ur = (low[a * T : (a + 1) * T] for a in range(4))
        allowed = causal & (label_col[h] == label_row[h])
        scores = jnp.where(allowed, nt(qr, kr) * factor, MASKED)
        raised = jnp.exp(scores - jnp.max(scores, axis=1, keepdims=True))
        weights = raised / jnp.sum(raised, axis=1, keepdims=True)
        weights_low = weights.astype(BF16)
        attended = nn(weights_low, vr).astype(BF16)
        row_dot = jnp.sum(u_wide * attended.astype(F32), axis=1, keepdims=True)
        grad_weights = nt(ur, vr)
        grad_scores = (weights * (grad_weights - row_dot) * factor).astype(BF16)
        grad_q = nn(grad_scores, kr).astype(BF16)
        grad_k = tn(grad_scores, qr).astype(BF16)
        grad_v = tn(weights_low, ur).astype(BF16)
        back = nn(permt[...], jnp.concatenate([attended, grad_q, grad_k, grad_v], axis=0))
        b_send[h] = back.reshape(NS, 8, HD).astype(BF16)
        b_recv[h, me] = b_send[h, me]
        send_all(lambda p: b_send.at[h, p], b_recv.at[h], b_ss.at[h], b_rs.at[h])
        unit = k_wide * lax.rsqrt(jnp.sum(k_wide * k_wide, axis=1, keepdims=True) + EPSILON)
        lead_sum = jnp.sum(unit * label_col[h], axis=0, keepdims=True)
        other_sum = jnp.sum(unit * (1.0 - label_col[h]), axis=0, keepdims=True)
        current = cen_s[h]
        for chosen, total in ((pick_lead[h], lead_sum), (pick_other[h], other_sum)):
            blended = RETAIN * jnp.sum(current * chosen, axis=0, keepdims=True) + (1.0 - RETAIN) * total
            renewed_rows.append(
                blended * lax.rsqrt(jnp.sum(blended * blended, axis=1, keepdims=True) + EPSILON)
            )
    cen_own = jnp.concatenate(renewed_rows, axis=0).astype(BF16)
    cen_send[...] = cen_own
    cen_recv[me] = cen_own
    send_all(lambda p: cen_send, cen_recv, cen_ss, cen_rs)

    q_inner = jnp.zeros((T, 1), F32)
    k_inner = jnp.zeros((T, 1), F32)
    for h in range(HL):
        cols = slice(h * HD, (h + 1) * HD)
        wait_blocks(b_recv.at[h], NS - 1, b_rs.at[h])
        received = b_recv[h].astype(F32).reshape(ROWS, HD).astype(BF16)
        home = nn(oht[h], received)
        att_o[:, cols] = home[0:T].astype(BF16)
        gv_o[:, cols] = home[3 * T : 4 * T].astype(BF16)
        gql_s[:, cols] = home[T : 2 * T]
        gkl_s[:, cols] = home[2 * T : 3 * T]
        q_inner += jnp.sum(home[T : 2 * T] * qn_s[:, cols], axis=1, keepdims=True)
        k_inner += jnp.sum(home[2 * T : 3 * T] * kn_s[:, cols], axis=1, keepdims=True)
    in_own = jnp.concatenate([to_row(q_inner, eye), to_row(k_inner, eye), jnp.zeros((6, T), F32)], axis=0)
    in_send[...] = in_own
    in_recv[hme] = in_own
    send_heads(in_send, in_recv, in_ss, in_rs)

    wait_blocks(cen_recv, NS - 1, cen_rs)
    renewed = cen_recv[...].astype(F32).reshape(ROWS, HD).astype(BF16)
    for h in range(HL):
        gather = (iota((C, ROWS), 1) == renewed_at[h]).astype(F32).astype(BF16)
        cen_o[h] = nn(gather, renewed)

    wait_blocks(in_recv, NH - 1, in_rs)
    inner = jnp.sum(in_recv[...], axis=0) * (1.0 / WIDTH)
    q_in = to_col(inner[0:1, :], eye)
    k_in = to_col(inner[1:2, :], eye)
    gq_o[...] = (q_scale * (gql_s[...] - qn_s[...] * q_in)).astype(BF16)
    gk_o[...] = (k_scale * (gkl_s[...] - kn_s[...] * k_in)).astype(BF16)

    wait_blocks(sq_recv, NH - 1, sq_ss)
    wait_blocks(in_recv, NH - 1, in_ss)
    wait_blocks(cnt_recv, NS - 1, cnt_ss)
    wait_blocks(cen_recv, NS - 1, cen_ss)
    for h in range(HL):
        wait_blocks(f_send.at[h], NS - 1, f_ss.at[h])
        wait_blocks(b_send.at[h], NS - 1, b_ss.at[h])


def local(query_vectors, key_vectors, value_vectors, cluster, centroids, upstream):
    wide = (T, HL * HD)
    blocks = (HL, NS, 8, HD)
    dma = pltpu.SemaphoreType.DMA
    return pl.pallas_call(
        kernel,
        out_shape=tuple(jax.ShapeDtypeStruct(wide, BF16) for _ in range(4))
        + (jax.ShapeDtypeStruct((HL, C, HD), F32),),
        in_specs=[pl.BlockSpec(memory_space=pl.ANY)] * 6,
        out_specs=tuple([pl.BlockSpec(memory_space=pltpu.VMEM)] * 5),
        scratch_shapes=[
            pltpu.VMEM(wide, BF16), pltpu.VMEM(wide, BF16), pltpu.VMEM(wide, BF16), pltpu.VMEM(wide, BF16),
            pltpu.VMEM((HL, T), jnp.int32), pltpu.VMEM((HL, C, HD), F32),
            pltpu.VMEM((HL, 4 * T, HD), BF16), pltpu.VMEM(wide, F32), pltpu.VMEM(wide, F32),
            pltpu.VMEM(wide, F32), pltpu.VMEM(wide, F32),
            pltpu.VMEM((ROWS, ROWS), BF16), pltpu.VMEM((ROWS, ROWS), BF16), pltpu.VMEM((HL, ROWS, ROWS), BF16),
            pltpu.VMEM((8, T), F32), pltpu.VMEM((NH, 8, T), F32),
            pltpu.VMEM((8, T), F32), pltpu.VMEM((NH, 8, T), F32),
            pltpu.VMEM((8, C), BF16), pltpu.VMEM((NS, 8, C), BF16),
            pltpu.VMEM((8, HD), BF16), pltpu.VMEM((NS, 8, HD), BF16),
            pltpu.VMEM(blocks, BF16), pltpu.VMEM(blocks, BF16), pltpu.VMEM(blocks, BF16), pltpu.VMEM(blocks, BF16),
            dma((6,)), dma, dma, dma, dma, dma, dma, dma, dma,
            dma((HL,)), dma((HL,)), dma((HL,)), dma((HL,)),
        ],
        compiler_params=pltpu.CompilerParams(collective_id=0, has_side_effects=True),
    )(query_vectors, key_vectors, value_vectors, upstream, cluster, centroids)


def solution(mesh):
    placed = (
        P("seq", "head"),
        P("seq", "head"),
        P("seq", "head"),
        P("head", "seq"),
        P("head", None, None),
        P("seq", "head"),
    )
    return jax.shard_map(
        local,
        mesh=mesh,
        in_specs=placed,
        out_specs=(
            P("seq", "head"),
            P("seq", "head"),
            P("seq", "head"),
            P("seq", "head"),
            P("head", None, None),
        ),
        check_vma=False,
    )
```

```python
import functools

import jax
import jax.numpy as jnp
from jax import lax
from jax.experimental import pallas as pl
from jax.experimental.pallas import tpu as pltpu
from jax.sharding import PartitionSpec as P

MASKED = -1e30
EPSILON = 1e-06
RETAIN = 0.9
MESH = pl.DeviceIdType.MESH
F32 = jnp.float32
BF16 = jnp.bfloat16

HD = 128
NS = 64
NX, NZ = 4, 16
NH = 8
HL = 4
T = 128
C = 128
WIDTH = 4096
ROWS = NS * 8


def iota(shape, dim):
    return lax.broadcasted_iota(jnp.int32, shape, dim)


def nt(a, b):
    return lax.dot_general(a, b, (((1,), (1,)), ((), ())), preferred_element_type=F32)


def tn(a, b):
    return lax.dot_general(a, b, (((0,), (0,)), ((), ())), preferred_element_type=F32)


def nn(a, b):
    return lax.dot_general(a, b, (((1,), (0,)), ((), ())), preferred_element_type=F32)


def to_row(column, eye):
    return jnp.sum(eye * column, axis=0, keepdims=True)


def to_col(row, eye):
    return jnp.sum(eye * row, axis=1, keepdims=True)


def kernel(
    q_hbm, k_hbm, v_hbm, u_hbm, cl_hbm, cen_hbm,
    att_o, gq_o, gk_o, gv_o, cen_o,
    q_s, k_s, v_s, u_s, cl_s, cen_s,
    xs, qn_s, kn_s, gql_s, gkl_s, perm, permt, oht,
    sq_send, sq_recv, in_send, in_recv, cnt_send, cnt_recv, cen_send, cen_recv,
    f_send, f_recv, b_send, b_recv, w_send, w_recv,
    load_sem, sq_ss, sq_rs, in_ss, in_rs, cnt_ss, cnt_rs, cen_ss, cen_rs, cex_ss, cex_rs,
    f_ss, f_rs, b_ss, b_rs, w_ss, w_rs,
):
    me = lax.axis_index("seq")
    hme = lax.axis_index("head")
    my_x, my_z = me // NZ, me % NZ
    row_of = [((my_x + NX - 1 - e) % NX) * NZ for e in range(NX)]

    def each_peer(act):
        def step(j, carry):
            far = NZ // 2 - (j + 1) // 2
            z = (my_z + far * (2 * (j % 2) - 1) + NZ) % NZ
            for e in range(NX):
                act(row_of[e] + z)
            return carry

        lax.fori_loop(0, NZ - 1, step, 0)
        for e in range(NX - 1):
            act(row_of[e] + my_z)

    def each_head(act):
        def step(i, carry):
            act((hme + 1 + i) % NH)
            return carry

        lax.fori_loop(0, NH - 1, step, 0)

    barrier = pltpu.get_barrier_semaphore()
    each_peer(lambda p: pl.semaphore_signal(barrier, 1, device_id=(hme, p), device_id_type=MESH))
    each_head(lambda p: pl.semaphore_signal(barrier, 1, device_id=(p, me), device_id_type=MESH))

    loads = [
        pltpu.make_async_copy(src, dst, load_sem.at[n])
        for n, (src, dst) in enumerate(
            ((cl_hbm, cl_s), (q_hbm, q_s), (k_hbm, k_s), (v_hbm, v_s), (u_hbm, u_s), (cen_hbm, cen_s))
        )
    ]
    for load in loads:
        load.start()

    def send(src, dst, ss, rs, to):
        pltpu.make_async_remote_copy(
            src_ref=src, dst_ref=dst, send_sem=ss, recv_sem=rs, device_id=to, device_id_type=MESH
        ).start()

    def send_all(src_at, dst, ss, rs):
        each_peer(lambda p: send(src_at(p), dst.at[me], ss, rs, (hme, p)))

    def send_heads(src, dst, ss, rs):
        each_head(lambda p: send(src, dst.at[hme], ss, rs, (p, me)))

    def wait_blocks(buf, n, sem):
        part = buf.at[pl.ds(0, n)]
        pltpu.make_async_copy(part, part, sem).wait()

    ic = iota((T, T), 0)
    il = iota((T, T), 1)
    eye = (ic == il).astype(F32)
    before = (ic < il).astype(F32)
    after = (ic > il).astype(F32)

    loads[0].wait()
    member, cnt_col, earlier, cnt_rows = [], [], [], []
    for h in range(HL):
        m = (ic == cl_s[h : h + 1, :]).astype(F32)
        member.append(m)
        mb = m.astype(BF16)
        n = jnp.sum(m, axis=1, keepdims=True)
        cnt_col.append(n)
        cnt_rows.append(to_row(n, eye))
        earlier.append(jnp.sum(tn(mb, mb) * before, axis=0, keepdims=True))
    cnt_own = jnp.concatenate(cnt_rows, axis=0).astype(BF16)
    cnt_send[...] = cnt_own
    cnt_recv[me] = cnt_own

    loads[1].wait()
    loads[2].wait()
    qf = q_s[...].astype(F32)
    q_row = to_row(jnp.sum(qf * qf, axis=1, keepdims=True), eye)
    kf = k_s[...].astype(F32)
    k_row = to_row(jnp.sum(kf * kf, axis=1, keepdims=True), eye)
    sq_own = jnp.concatenate([q_row, k_row, jnp.zeros((6, T), F32)], axis=0)
    sq_send[...] = sq_own
    sq_recv[hme] = sq_own

    big_r = iota((ROWS, ROWS), 0)
    big_l = iota((ROWS, ROWS), 1)
    perm[...] = (big_r == ((big_l // 2) % 4) * T + (big_l // 8) * 2 + big_l % 2).astype(F32).astype(BF16)
    permt[...] = (big_l == ((big_r // 2) % 4) * T + (big_r // 8) * 2 + big_r % 2).astype(F32).astype(BF16)

    loads[3].wait()
    loads[4].wait()
    for h in range(HL):
        xs[h, 2 * T : 3 * T, :] = v_s[:, h * HD : (h + 1) * HD]
        xs[h, 3 * T : 4 * T, :] = u_s[:, h * HD : (h + 1) * HD]
    loads[5].wait()

    pl.semaphore_wait(barrier, NS - 1 + NH - 1)
    send_all(lambda p: cnt_send, cnt_recv, cnt_ss, cnt_rs)
    send_heads(sq_send, sq_recv, sq_ss, sq_rs)

    wait_blocks(sq_recv, NH - 1, sq_rs)
    squares = jnp.sum(sq_recv[...], axis=0)
    scales = lax.rsqrt(squares * (1.0 / WIDTH) + EPSILON)
    q_scale = to_col(scales[0:1, :], eye)
    k_scale = to_col(scales[1:2, :], eye)
    q_norm = q_s[...].astype(F32) * q_scale
    k_norm = k_s[...].astype(F32) * k_scale
    qn_s[...] = q_norm
    kn_s[...] = k_norm
    q_low = q_norm.astype(BF16)
    k_low = k_norm.astype(BF16)
    for h in range(HL):
        xs[h, 0:T, :] = q_low[:, h * HD : (h + 1) * HD]
        xs[h, T : 2 * T, :] = k_low[:, h * HD : (h + 1) * HD]

    wait_blocks(cnt_recv, NS - 1, cnt_rs)
    table = jnp.concatenate([cnt_recv[...].astype(F32), jnp.zeros((NS, 8 - HL, C), F32)], axis=1)
    table = table.reshape(ROWS, C).astype(BF16)
    slot = (iota((T, 1), 0) % 2).astype(F32)
    label_col, label_row, pick_lead, pick_other, renewed_at, place_col = [], [], [], [], [], []
    mine = me.astype(F32)
    for h in range(HL):
        g, half = h // 2, (h % 2) * 8
        spread = (iota((T, ROWS), 1) == (iota((T, ROWS), 0) // 2) * 8 + h).astype(F32).astype(BF16)
        counts = nn(spread, table)
        swing = counts - 1.0
        sb = swing.astype(BF16)
        gram = tn(sb, sb)
        n_row = jnp.sum(swing * swing, axis=0, keepdims=True)
        n_sum = n_row + to_col(n_row, eye)
        opposite = (n_sum + 2.0 * gram == 0.0).astype(F32)
        same = (n_sum - 2.0 * gram == 0.0).astype(F32)
        rank_row = jnp.sum(same * before, axis=0, keepdims=True)
        rank_col = jnp.sum(same * after, axis=1, keepdims=True)
        partner = jnp.where(rank_row == rank_col, opposite, 0.0)
        other_row = jnp.sum(partner * before, axis=0, keepdims=True)
        other_col = jnp.sum(partner * after, axis=1, keepdims=True)
        lead_rank_row = jnp.sum((1.0 - other_col) * before, axis=0, keepdims=True)
        lead_rank_col = jnp.sum((1.0 - other_row) * after, axis=1, keepdims=True)
        partner_rank_col = jnp.sum(partner * lead_rank_row, axis=1, keepdims=True)
        owner_col = jnp.where(other_col > 0.0, partner_rank_col, lead_rank_col)
        base = 8.0 * owner_col + other_col * (2.0 - cnt_col[h])
        place = jnp.sum(member[h] * base, axis=0, keepdims=True) + earlier[h]
        place_col.append(to_col(place, eye))
        target = jnp.concatenate([place + 2.0 * a for a in range(4)], axis=1).astype(jnp.int32)
        onehot = (big_r == target).astype(F32).astype(BF16)
        packed = nn(onehot, xs[h])
        f_send[g, :, half : half + 8, :] = packed.reshape(NS, 8, HD).astype(BF16)
        if half:
            f_recv[g, me] = f_send[g, me]
            send_all(lambda p: f_send.at[g, p], f_recv.at[g], f_ss.at[g], f_rs.at[g])
        lead_mine_row = jnp.where((other_row == 0.0) & (lead_rank_row == mine), 1.0, 0.0)
        lead_count = jnp.sum(counts * lead_mine_row, axis=1, keepdims=True)
        label = (slot < lead_count).astype(F32)
        label_col.append(label)
        label_row.append(to_row(label, eye))
        pick_lead.append(jnp.where((other_col == 0.0) & (owner_col == mine), 1.0, 0.0))
        pick_other.append(jnp.where((other_col > 0.0) & (owner_col == mine), 1.0, 0.0))
        renewed_at.append((owner_col * 8.0 + (2.0 * h) + other_col).astype(jnp.int32))

    for h in range(HL):
        for a in range(4):
            oht[h, a * T : (a + 1) * T, :] = (
                (iota((T, ROWS), 1) == (place_col[h] + 2.0 * a).astype(jnp.int32)).astype(F32).astype(BF16)
            )

    factor = HD ** (-0.5)
    causal = il <= ic

    def attend(h, received):
        rows = nn(perm[...], received)
        k_wide = rows[T : 2 * T]
        u_wide = rows[3 * T : 4 * T]
        low = rows.astype(BF16)
        qr, kr, vr, ur = (low[a * T : (a + 1) * T] for a in range(4))
        allowed = causal & (label_col[h] == label_row[h])
        scores = jnp.where(allowed, nt(qr, kr) * factor, MASKED)
        raised = jnp.exp(scores - jnp.max(scores, axis=1, keepdims=True))
        weights = raised / jnp.sum(raised, axis=1, keepdims=True)
        weights_low = weights.astype(BF16)
        attended = nn(weights_low, vr).astype(BF16)
        row_dot = jnp.sum(u_wide * attended.astype(F32), axis=1, keepdims=True)
        grad_weights = nt(ur, vr)
        grad_scores = (weights * (grad_weights - row_dot) * factor).astype(BF16)
        grad_q = nn(grad_scores, kr).astype(BF16)
        grad_k = tn(grad_scores, qr).astype(BF16)
        grad_v = tn(weights_low, ur).astype(BF16)
        unit = k_wide * lax.rsqrt(jnp.sum(k_wide * k_wide, axis=1, keepdims=True) + EPSILON)
        lead_sum = jnp.sum(unit * label_col[h], axis=0, keepdims=True)
        other_sum = jnp.sum(unit * (1.0 - label_col[h]), axis=0, keepdims=True)
        current = cen_s[h]
        renewed = []
        for chosen, total in ((pick_lead[h], lead_sum), (pick_other[h], other_sum)):
            blended = RETAIN * jnp.sum(current * chosen, axis=0, keepdims=True) + (1.0 - RETAIN) * total
            renewed.append(blended * lax.rsqrt(jnp.sum(blended * blended, axis=1, keepdims=True) + EPSILON))
        return attended, grad_q, grad_k, grad_v, renewed

    def by_device(arrays):
        return nn(permt[...], jnp.concatenate(arrays, axis=0)).reshape(NS, 8, HD).astype(BF16)

    def arrived(part):
        return part.astype(F32).reshape(ROWS, HD).astype(BF16)

    wait_blocks(f_recv.at[0], NS - 1, f_rs.at[0])
    cen_rows = []
    for h in range(2):
        attended, grad_q, grad_k, grad_v, renewed = attend(h, arrived(f_recv[0, :, h * 8 : h * 8 + 8, :]))
        cen_rows += renewed
        b_send[:, h * 8 : h * 8 + 8, :] = by_device([attended, grad_q, grad_k, grad_v])
    b_recv[me] = b_send[me]
    send_all(lambda p: b_send.at[p], b_recv, b_ss, b_rs)

    wait_blocks(f_recv.at[1], NS - 1, f_rs.at[1])
    first, second = [], []
    for h in range(2):
        attended, grad_q, grad_k, grad_v, renewed = attend(h + 2, arrived(f_recv[1, :, h * 8 : h * 8 + 8, :]))
        cen_rows += renewed
        first += [grad_q, grad_k]
        second += [attended, grad_v]
    cen_own = jnp.concatenate(cen_rows, axis=0).astype(BF16)
    cen_send[...] = cen_own
    cen_recv[my_x, my_z] = cen_own
    w_send[0] = by_device(first)
    w_recv[0, me] = w_send[0, me]

    def cen_along_z(i, carry):
        send(cen_send, cen_recv.at[my_x, my_z], cen_ss, cen_rs, (hme, my_x * NZ + (my_z + 1 + i) % NZ))
        return carry

    lax.fori_loop(0, NZ - 1, cen_along_z, 0)
    send_all(lambda p: w_send.at[0, p], w_recv.at[0], w_ss.at[0], w_rs.at[0])
    w_send[1] = by_device(second)
    w_recv[1, me] = w_send[1, me]
    send_all(lambda p: w_send.at[1, p], w_recv.at[1], w_ss.at[1], w_rs.at[1])

    q_inner = jnp.zeros((T, 1), F32)
    k_inner = jnp.zeros((T, 1), F32)

    def keep_grads(h, grad_q, grad_k, q_sum, k_sum):
        cols = slice(h * HD, (h + 1) * HD)
        gql_s[:, cols] = grad_q
        gkl_s[:, cols] = grad_k
        return (
            q_sum + jnp.sum(grad_q * qn_s[:, cols], axis=1, keepdims=True),
            k_sum + jnp.sum(grad_k * kn_s[:, cols], axis=1, keepdims=True),
        )

    wait_blocks(b_recv, NS - 1, b_rs)
    for h in range(2):
        cols = slice(h * HD, (h + 1) * HD)
        home = nn(oht[h], arrived(b_recv[:, h * 8 : h * 8 + 8, :]))
        att_o[:, cols] = home[0:T].astype(BF16)
        gv_o[:, cols] = home[3 * T : 4 * T].astype(BF16)
        q_inner, k_inner = keep_grads(h, home[T : 2 * T], home[2 * T : 3 * T], q_inner, k_inner)

    wait_blocks(cen_recv.at[my_x], NZ - 1, cen_rs)
    for e in range(NX - 1):
        send(cen_recv.at[my_x], cen_recv.at[my_x], cex_ss, cex_rs, (hme, row_of[e] + my_z))

    wait_blocks(w_recv.at[0], NS - 1, w_rs.at[0])
    received = arrived(w_recv[0])
    for h in range(2, HL):
        two = slice((h - 2) * 2 * T, (h - 1) * 2 * T)
        home = nn(oht[h, two, :], received)
        q_inner, k_inner = keep_grads(h, home[0:T], home[T : 2 * T], q_inner, k_inner)
    in_own = jnp.concatenate([to_row(q_inner, eye), to_row(k_inner, eye), jnp.zeros((6, T), F32)], axis=0)
    in_send[...] = in_own
    in_recv[hme] = in_own
    send_heads(in_send, in_recv, in_ss, in_rs)

    wait_blocks(cen_recv, NX - 1, cex_rs)
    renewed = cen_recv[...].astype(F32).reshape(ROWS, HD).astype(BF16)
    for h in range(HL):
        gather = (iota((C, ROWS), 1) == renewed_at[h]).astype(F32).astype(BF16)
        cen_o[h] = nn(gather, renewed)

    wait_blocks(in_recv, NH - 1, in_rs)
    inner = jnp.sum(in_recv[...], axis=0) * (1.0 / WIDTH)
    q_in = to_col(inner[0:1, :], eye)
    k_in = to_col(inner[1:2, :], eye)
    gq_o[...] = (q_scale * (gql_s[...] - qn_s[...] * q_in)).astype(BF16)
    gk_o[...] = (k_scale * (gkl_s[...] - kn_s[...] * k_in)).astype(BF16)

    wait_blocks(sq_recv, NH - 1, sq_ss)
    wait_blocks(in_recv, NH - 1, in_ss)
    wait_blocks(cnt_recv, NS - 1, cnt_ss)
    wait_blocks(cen_recv.at[my_x], NZ - 1, cen_ss)
    wait_blocks(cen_recv, NX - 1, cex_ss)
    for g in range(2):
        wait_blocks(f_send.at[g], NS - 1, f_ss.at[g])
        wait_blocks(w_send.at[g], NS - 1, w_ss.at[g])
    wait_blocks(b_send, NS - 1, b_ss)

    wait_blocks(w_recv.at[1], NS - 1, w_rs.at[1])
    received = arrived(w_recv[1])
    for h in range(2, HL):
        cols = slice(h * HD, (h + 1) * HD)
        two = slice((h - 2) * 2 * T, (h - 1) * 2 * T)
        home = nn(oht[h, two, :], received)
        att_o[:, cols] = home[0:T].astype(BF16)
        gv_o[:, cols] = home[T : 2 * T].astype(BF16)


def put_out(*refs):
    n = len(refs) // 2
    sems = refs[-1]
    copies = [pltpu.make_async_copy(refs[i], refs[n + i], sems.at[i]) for i in range(n)]
    for copy in copies:
        copy.start()
    for copy in copies:
        copy.wait()


def local(query_vectors, key_vectors, value_vectors, cluster, centroids, upstream):
    wide = (T, HL * HD)
    dma = pltpu.SemaphoreType.DMA
    held = pl.pallas_call(
        kernel,
        out_shape=tuple(pltpu.VMEM(wide, BF16) for _ in range(4)) + (pltpu.VMEM((HL, C, HD), F32),),
        in_specs=[pl.BlockSpec(memory_space=pl.ANY)] * 6,
        out_specs=tuple([pl.BlockSpec(memory_space=pltpu.VMEM)] * 5),
        scratch_shapes=[
            pltpu.VMEM(wide, BF16), pltpu.VMEM(wide, BF16), pltpu.VMEM(wide, BF16), pltpu.VMEM(wide, BF16),
            pltpu.VMEM((HL, T), jnp.int32), pltpu.VMEM((HL, C, HD), F32),
            pltpu.VMEM((HL, 4 * T, HD), BF16), pltpu.VMEM(wide, F32), pltpu.VMEM(wide, F32),
            pltpu.VMEM(wide, F32), pltpu.VMEM(wide, F32),
            pltpu.VMEM((ROWS, ROWS), BF16), pltpu.VMEM((ROWS, ROWS), BF16), pltpu.VMEM((HL, ROWS, ROWS), BF16),
            pltpu.VMEM((8, T), F32), pltpu.VMEM((NH, 8, T), F32),
            pltpu.VMEM((8, T), F32), pltpu.VMEM((NH, 8, T), F32),
            pltpu.VMEM((HL, C), BF16), pltpu.VMEM((NS, HL, C), BF16),
            pltpu.VMEM((8, HD), BF16), pltpu.VMEM((NX, NZ, 8, HD), BF16),
            pltpu.VMEM((2, NS, 16, HD), BF16), pltpu.VMEM((2, NS, 16, HD), BF16),
            pltpu.VMEM((NS, 16, HD), BF16), pltpu.VMEM((NS, 16, HD), BF16),
            pltpu.VMEM((2, NS, 8, HD), BF16), pltpu.VMEM((2, NS, 8, HD), BF16),
            dma((6,)), dma, dma, dma, dma, dma, dma, dma, dma, dma, dma,
            dma((2,)), dma((2,)), dma, dma, dma((2,)), dma((2,)),
        ],
        compiler_params=pltpu.CompilerParams(collective_id=0, has_side_effects=True),
    )(query_vectors, key_vectors, value_vectors, upstream, cluster, centroids)
    return pl.pallas_call(
        put_out,
        out_shape=tuple(jax.ShapeDtypeStruct(wide, BF16) for _ in range(4))
        + (jax.ShapeDtypeStruct((HL, C, HD), F32),),
        in_specs=[pl.BlockSpec(memory_space=pltpu.VMEM)] * 5,
        out_specs=tuple([pl.BlockSpec(memory_space=pl.ANY)] * 5),
        scratch_shapes=[dma((5,))],
    )(*(pltpu.with_memory_space_constraint(one, pltpu.VMEM) for one in held))


def solution(mesh):
    placed = (
        P("seq", "head"),
        P("seq", "head"),
        P("seq", "head"),
        P("head", "seq"),
        P("head", None, None),
        P("seq", "head"),
    )
    return jax.shard_map(
        local,
        mesh=mesh,
        in_specs=placed,
        out_specs=(
            P("seq", "head"),
            P("seq", "head"),
            P("seq", "head"),
            P("seq", "head"),
            P("head", None, None),
        ),
        check_vma=False,
    )
```

```python
import functools

import jax
import jax.numpy as jnp
from jax import lax
from jax.experimental import pallas as pl
from jax.experimental.pallas import tpu as pltpu
from jax.sharding import PartitionSpec as P

MASKED = -1e30
EPSILON = 1e-06
RETAIN = 0.9
MESH = pl.DeviceIdType.MESH
F32 = jnp.float32
BF16 = jnp.bfloat16

HD = 128
NS = 64
NX, NZ = 4, 16
NH = 8
HL = 4
T = 128
C = 128
WIDTH = 4096
NEAR = 4
SPLIT = 3
LATER = 5
ROWS = NS * 8


def iota(shape, dim):
    return lax.broadcasted_iota(jnp.int32, shape, dim)


def nt(a, b):
    return lax.dot_general(a, b, (((1,), (1,)), ((), ())), preferred_element_type=F32)


def tn(a, b):
    return lax.dot_general(a, b, (((0,), (0,)), ((), ())), preferred_element_type=F32)


def nn(a, b):
    return lax.dot_general(a, b, (((1,), (0,)), ((), ())), preferred_element_type=F32)


def to_row(column, eye):
    return jnp.sum(eye * column, axis=0, keepdims=True)


def to_col(row, eye):
    return jnp.sum(eye * row, axis=1, keepdims=True)


def kernel(
    q_hbm, k_hbm, v_hbm, u_hbm, cl_hbm, cen_hbm,
    att_o, gq_o, gk_o, gv_o, cen_o,
    q_s, k_s, v_s, u_s, cl_s, cen_s,
    xs, qn_s, kn_s, gql_s, gkl_s, perm, permt, oht,
    sq_send, sq_recv, in_send, in_recv, cnt_send, cnt_recv, cen_send, cen_recv,
    f_send, f_recv, w_send, w_recv,
    load_sem, sq_ss, sq_rs, in_ss, in_rs, cnt_ss, cnt_rs, cen_ss, cen_rs, cex_ss, cex_rs,
    f_ss, f_rs, w_ss, w_rs,
):
    me = lax.axis_index("seq")
    hme = lax.axis_index("head")
    my_x, my_z = me // NZ, me % NZ
    row_of = [((my_x + NX - 1 - e) % NX) * NZ for e in range(NX)]

    def each_peer(act, begin=0, end=NZ):
        def step(j, carry):
            far = NZ // 2 - (j + 1) // 2
            z = (my_z + far * (2 * (j % 2) - 1) + NZ) % NZ
            for e in range(NX):
                act(row_of[e] + z)
            return carry

        lax.fori_loop(begin, min(end, NZ - 1), step, 0)
        if end == NZ:
            for e in range(NX - 1):
                act(row_of[e] + my_z)

    def each_head(act):
        def step(i, carry):
            act((hme + 1 + i) % NH)
            return carry

        lax.fori_loop(0, NH - 1, step, 0)

    barrier = pltpu.get_barrier_semaphore()

    def greet(to):
        pl.semaphore_signal(barrier, 1, device_id=to, device_id_type=MESH)

    for d in range(NEAR, 0, -1):
        for side in (d, NZ - d):
            greet((hme, my_x * NZ + (my_z + side) % NZ))
    for e in range(NX - 1):
        greet((hme, row_of[e] + my_z))
    each_head(lambda p: greet((p, me)))

    loads = [
        pltpu.make_async_copy(src, dst, load_sem.at[n])
        for n, (src, dst) in enumerate(
            ((cl_hbm, cl_s), (q_hbm, q_s), (k_hbm, k_s), (v_hbm, v_s), (u_hbm, u_s), (cen_hbm, cen_s))
        )
    ]
    for load in loads:
        load.start()

    def send(src, dst, ss, rs, to):
        pltpu.make_async_remote_copy(
            src_ref=src, dst_ref=dst, send_sem=ss, recv_sem=rs, device_id=to, device_id_type=MESH
        ).start()

    def send_all(src_at, dst, ss, rs, begin=0, end=NZ):
        each_peer(lambda p: send(src_at(p), dst.at[me], ss, rs, (hme, p)), begin, end)

    def send_heads(src, dst, ss, rs):
        each_head(lambda p: send(src, dst.at[hme], ss, rs, (p, me)))

    def wait_blocks(buf, n, sem):
        part = buf.at[pl.ds(0, n)]
        pltpu.make_async_copy(part, part, sem).wait()

    ic = iota((T, T), 0)
    il = iota((T, T), 1)
    eye = (ic == il).astype(F32)
    before = (ic < il).astype(F32)
    after = (ic > il).astype(F32)

    loads[0].wait()
    member, cnt_col, earlier, cnt_rows = [], [], [], []
    for h in range(HL):
        m = (ic == cl_s[h : h + 1, :]).astype(F32)
        member.append(m)
        mb = m.astype(BF16)
        n = jnp.sum(m, axis=1, keepdims=True)
        cnt_col.append(n)
        cnt_rows.append(to_row(n, eye))
        earlier.append(jnp.sum(tn(mb, mb) * before, axis=0, keepdims=True))
    cnt_own = jnp.concatenate(cnt_rows, axis=0).astype(BF16)
    cnt_send[...] = cnt_own
    cnt_recv[my_x, my_z] = cnt_own

    loads[1].wait()
    loads[2].wait()
    qf = q_s[...].astype(F32)
    q_row = to_row(jnp.sum(qf * qf, axis=1, keepdims=True), eye)
    kf = k_s[...].astype(F32)
    k_row = to_row(jnp.sum(kf * kf, axis=1, keepdims=True), eye)
    sq_own = jnp.concatenate([q_row, k_row], axis=0)
    sq_send[...] = sq_own
    sq_recv[hme] = sq_own

    big_r = iota((ROWS, ROWS), 0)
    big_l = iota((ROWS, ROWS), 1)
    perm[...] = (big_r == ((big_l // 2) % 4) * T + (big_l // 8) * 2 + big_l % 2).astype(F32).astype(BF16)
    permt[...] = (big_l == ((big_r // 2) % 4) * T + (big_r // 8) * 2 + big_r % 2).astype(F32).astype(BF16)

    loads[3].wait()
    loads[4].wait()
    for h in range(HL):
        xs[h, 2 * T : 3 * T, :] = v_s[:, h * HD : (h + 1) * HD]
        xs[h, 3 * T : 4 * T, :] = u_s[:, h * HD : (h + 1) * HD]
    loads[5].wait()

    pl.semaphore_wait(barrier, 2 * NEAR + NX - 1 + NH - 1)
    for d in range(NEAR, 0, -1):
        for side in (d, NZ - d):
            to = (hme, my_x * NZ + (my_z + side) % NZ)
            send(cnt_send, cnt_recv.at[my_x, my_z], cnt_ss.at[0], cnt_rs.at[0], to)
    send_heads(sq_send, sq_recv, sq_ss, sq_rs)

    def normalize():
        wait_blocks(sq_recv, NH - 1, sq_rs)
        squares = jnp.sum(sq_recv[...], axis=0)
        scales = lax.rsqrt(squares * (1.0 / WIDTH) + EPSILON)
        q_scale = to_col(scales[0:1, :], eye)
        k_scale = to_col(scales[1:2, :], eye)
        q_norm = q_s[...].astype(F32) * q_scale
        k_norm = k_s[...].astype(F32) * k_scale
        qn_s[...] = q_norm
        kn_s[...] = k_norm
        q_low = q_norm.astype(BF16)
        k_low = k_norm.astype(BF16)
        for h in range(HL):
            xs[h, 0:T, :] = q_low[:, h * HD : (h + 1) * HD]
            xs[h, T : 2 * T, :] = k_low[:, h * HD : (h + 1) * HD]
        return q_scale, k_scale

    wait_blocks(cnt_recv.at[0], 2 * NEAR, cnt_rs.at[0])
    for side, rows in ((NZ - NEAR, range(NEAR, 0, -1)), (NEAR, range(NZ - NEAR + 1, NZ))):
        to = (hme, my_x * NZ + (my_z + side) % NZ)
        for r in rows:
            part = cnt_recv.at[my_x, (my_z + r) % NZ]
            send(part, part, cnt_ss.at[1], cnt_rs.at[1], to)
    q_scale, k_scale = normalize()
    wait_blocks(cnt_recv.at[0], 2 * NEAR - 1, cnt_rs.at[1])
    for e in range(NX - 1):
        send(cnt_recv.at[my_x], cnt_recv.at[my_x], cnt_ss.at[2], cnt_rs.at[2], (hme, row_of[e] + my_z))
    wait_blocks(cnt_recv, NX - 1, cnt_rs.at[2])
    table = cnt_recv[...].astype(F32).reshape(NS, HL, C)
    table = jnp.concatenate([table, jnp.zeros((NS, 8 - HL, C), F32)], axis=1)
    table = table.reshape(ROWS, C).astype(BF16)
    slot = (iota((T, 1), 0) % 2).astype(F32)
    label_col, label_row, pick_lead, pick_other, renewed_at, place_col = [], [], [], [], [], []
    mine = me.astype(F32)
    for h in range(HL):
        g, half = h // 2, (h % 2) * 8
        spread = (iota((T, ROWS), 1) == (iota((T, ROWS), 0) // 2) * 8 + h).astype(F32).astype(BF16)
        counts = nn(spread, table)
        swing = counts - 1.0
        sb = swing.astype(BF16)
        gram = tn(sb, sb)
        n_row = jnp.sum(swing * swing, axis=0, keepdims=True)
        n_sum = n_row + to_col(n_row, eye)
        opposite = (n_sum + 2.0 * gram == 0.0).astype(F32)
        same = (n_sum - 2.0 * gram == 0.0).astype(F32)
        rank_row = jnp.sum(same * before, axis=0, keepdims=True)
        rank_col = jnp.sum(same * after, axis=1, keepdims=True)
        partner = jnp.where(rank_row == rank_col, opposite, 0.0)
        other_row = jnp.sum(partner * before, axis=0, keepdims=True)
        other_col = jnp.sum(partner * after, axis=1, keepdims=True)
        lead_rank_row = jnp.sum((1.0 - other_col) * before, axis=0, keepdims=True)
        lead_rank_col = jnp.sum((1.0 - other_row) * after, axis=1, keepdims=True)
        partner_rank_col = jnp.sum(partner * lead_rank_row, axis=1, keepdims=True)
        owner_col = jnp.where(other_col > 0.0, partner_rank_col, lead_rank_col)
        base = 8.0 * owner_col + other_col * (2.0 - cnt_col[h])
        place = jnp.sum(member[h] * base, axis=0, keepdims=True) + earlier[h]
        place_col.append(to_col(place, eye))
        target = jnp.concatenate([place + 2.0 * a for a in range(4)], axis=1).astype(jnp.int32)
        onehot = (big_r == target).astype(F32).astype(BF16)
        packed = nn(onehot, xs[h])
        f_send[g, :, half : half + 8, :] = packed.reshape(NS, 8, HD).astype(BF16)
        if half:
            f_recv[g, me] = f_send[g, me]
            send_all(lambda p: f_send.at[g, p], f_recv.at[g], f_ss.at[g], f_rs.at[g])
        lead_mine_row = jnp.where((other_row == 0.0) & (lead_rank_row == mine), 1.0, 0.0)
        lead_count = jnp.sum(counts * lead_mine_row, axis=1, keepdims=True)
        label = (slot < lead_count).astype(F32)
        label_col.append(label)
        label_row.append(to_row(label, eye))
        pick_lead.append(jnp.where((other_col == 0.0) & (owner_col == mine), 1.0, 0.0))
        pick_other.append(jnp.where((other_col > 0.0) & (owner_col == mine), 1.0, 0.0))
        renewed_at.append((owner_col * 8.0 + (2.0 * h) + other_col).astype(jnp.int32))

    for h in range(HL):
        for a in range(4):
            oht[h, a * T : (a + 1) * T, :] = (
                (iota((T, ROWS), 1) == (place_col[h] + 2.0 * a).astype(jnp.int32)).astype(F32).astype(BF16)
            )

    factor = HD ** (-0.5)
    causal = il <= ic

    def attend(h, received):
        rows = nn(perm[...], received)
        k_wide = rows[T : 2 * T]
        u_wide = rows[3 * T : 4 * T]
        low = rows.astype(BF16)
        qr, kr, vr, ur = (low[a * T : (a + 1) * T] for a in range(4))
        allowed = causal & (label_col[h] == label_row[h])
        scores = jnp.where(allowed, nt(qr, kr) * factor, MASKED)
        raised = jnp.exp(scores - jnp.max(scores, axis=1, keepdims=True))
        weights = raised / jnp.sum(raised, axis=1, keepdims=True)
        weights_low = weights.astype(BF16)
        attended = nn(weights_low, vr).astype(BF16)
        row_dot = jnp.sum(u_wide * attended.astype(F32), axis=1, keepdims=True)
        grad_weights = nt(ur, vr)
        grad_scores = (weights * (grad_weights - row_dot) * factor).astype(BF16)
        grad_q = nn(grad_scores, kr).astype(BF16)
        grad_k = tn(grad_scores, qr).astype(BF16)
        grad_v = tn(weights_low, ur).astype(BF16)
        unit = k_wide * lax.rsqrt(jnp.sum(k_wide * k_wide, axis=1, keepdims=True) + EPSILON)
        lead_sum = jnp.sum(unit * label_col[h], axis=0, keepdims=True)
        other_sum = jnp.sum(unit * (1.0 - label_col[h]), axis=0, keepdims=True)
        current = cen_s[h]
        renewed = []
        for chosen, total in ((pick_lead[h], lead_sum), (pick_other[h], other_sum)):
            blended = RETAIN * jnp.sum(current * chosen, axis=0, keepdims=True) + (1.0 - RETAIN) * total
            renewed.append(blended * lax.rsqrt(jnp.sum(blended * blended, axis=1, keepdims=True) + EPSILON))
        return attended, grad_q, grad_k, grad_v, renewed

    def by_device(arrays):
        return nn(permt[...], jnp.concatenate(arrays, axis=0)).reshape(NS, 8, HD).astype(BF16)

    def arrived(part):
        return part.astype(F32).reshape(ROWS, HD).astype(BF16)

    def put_back(n, arrays):
        w_send[n] = by_device(arrays)
        w_recv[n, me] = w_send[n, me]

    def send_back(n, begin=0, end=NZ):
        send_all(lambda p: w_send.at[n, p], w_recv.at[n], w_ss.at[n], w_rs.at[n], begin, end)

    cen_rows = []
    for g in range(2):
        wait_blocks(f_recv.at[g], NS - 1, f_rs.at[g])
        first, second = [], []
        for half in range(2):
            attended, grad_q, grad_k, grad_v, renewed = attend(
                2 * g + half, arrived(f_recv[g, :, half * 8 : half * 8 + 8, :])
            )
            cen_rows += renewed
            first += [grad_q, grad_k]
            second += [attended, grad_v]
        put_back(g, first)
        send_back(g)
        put_back(2 + g, second)
        if g == 0:
            send_back(2, 0, SPLIT)
    cen_own = jnp.concatenate(cen_rows, axis=0).astype(BF16)
    cen_send[...] = cen_own
    cen_recv[my_x, my_z] = cen_own

    def cen_along_z(i, carry):
        far = NZ // 2 - (i + 1) // 2
        z = (my_z + far * (2 * (i % 2) - 1) + NZ) % NZ
        send(cen_send, cen_recv.at[my_x, my_z], cen_ss, cen_rs, (hme, my_x * NZ + z))
        return carry

    lax.fori_loop(0, NZ - 1, cen_along_z, 0)
    send_back(2, SPLIT, NZ)

    inner_sums = [jnp.zeros((T, 1), F32), jnp.zeros((T, 1), F32)]

    def home_grads(g, received):
        for half in range(2):
            h = 2 * g + half
            cols = slice(h * HD, (h + 1) * HD)
            home = nn(oht[h, half * 2 * T : (half + 1) * 2 * T, :], received)
            gql_s[:, cols] = home[0:T]
            gkl_s[:, cols] = home[T : 2 * T]
            inner_sums[0] += jnp.sum(home[0:T] * qn_s[:, cols], axis=1, keepdims=True)
            inner_sums[1] += jnp.sum(home[T : 2 * T] * kn_s[:, cols], axis=1, keepdims=True)

    def home_values(g, received):
        for half in range(2):
            h = 2 * g + half
            cols = slice(h * HD, (h + 1) * HD)
            home = nn(oht[h, half * 2 * T : (half + 1) * 2 * T, :], received)
            att_o[:, cols] = home[0:T].astype(BF16)
            gv_o[:, cols] = home[T : 2 * T].astype(BF16)

    wait_blocks(w_recv.at[0], NS - 1, w_rs.at[0])
    home_grads(0, arrived(w_recv[0]))
    wait_blocks(w_recv.at[1], NS - 1, w_rs.at[1])
    home_grads(1, arrived(w_recv[1]))
    in_own = jnp.concatenate([to_row(inner_sums[0], eye), to_row(inner_sums[1], eye)], axis=0)
    in_send[...] = in_own
    in_recv[hme] = in_own
    send_heads(in_send, in_recv, in_ss, in_rs)
    send_back(3, 0, LATER)

    wait_blocks(cen_recv.at[my_x], NZ - 1, cen_rs)
    for e in range(NX - 1):
        send(cen_recv.at[my_x], cen_recv.at[my_x], cex_ss, cex_rs, (hme, row_of[e] + my_z))
    send_back(3, LATER, NZ)
    wait_blocks(w_recv.at[2], NS - 1, w_rs.at[2])
    home_values(0, arrived(w_recv[2]))

    wait_blocks(cen_recv, NX - 1, cex_rs)
    renewed = cen_recv[...].astype(F32).reshape(ROWS, HD).astype(BF16)
    for h in range(HL):
        gather = (iota((C, ROWS), 1) == renewed_at[h]).astype(F32).astype(BF16)
        cen_o[h] = nn(gather, renewed)

    wait_blocks(in_recv, NH - 1, in_rs)
    inner = jnp.sum(in_recv[...], axis=0) * (1.0 / WIDTH)
    q_in = to_col(inner[0:1, :], eye)
    k_in = to_col(inner[1:2, :], eye)
    gq_o[...] = (q_scale * (gql_s[...] - qn_s[...] * q_in)).astype(BF16)
    gk_o[...] = (k_scale * (gkl_s[...] - kn_s[...] * k_in)).astype(BF16)

    wait_blocks(sq_recv, NH - 1, sq_ss)
    wait_blocks(in_recv, NH - 1, in_ss)
    wait_blocks(cnt_recv.at[0], 2 * NEAR, cnt_ss.at[0])
    wait_blocks(cnt_recv.at[0], 2 * NEAR - 1, cnt_ss.at[1])
    wait_blocks(cnt_recv, NX - 1, cnt_ss.at[2])
    wait_blocks(cen_recv.at[my_x], NZ - 1, cen_ss)
    wait_blocks(cen_recv, NX - 1, cex_ss)
    for g in range(2):
        wait_blocks(f_send.at[g], NS - 1, f_ss.at[g])

    for n in range(3):
        wait_blocks(w_send.at[n], NS - 1, w_ss.at[n])

    wait_blocks(w_recv.at[3], NS - 1, w_rs.at[3])
    home_values(1, arrived(w_recv[3]))
    wait_blocks(w_send.at[3], NS - 1, w_ss.at[3])


def put_out(*refs):
    n = len(refs) // 2
    sems = refs[-1]
    copies = [pltpu.make_async_copy(refs[i], refs[n + i], sems.at[i]) for i in range(n)]
    for copy in copies:
        copy.start()
    for copy in copies:
        copy.wait()


def local(query_vectors, key_vectors, value_vectors, cluster, centroids, upstream):
    wide = (T, HL * HD)
    dma = pltpu.SemaphoreType.DMA
    held = pl.pallas_call(
        kernel,
        out_shape=tuple(pltpu.VMEM(wide, BF16) for _ in range(4)) + (pltpu.VMEM((HL, C, HD), F32),),
        in_specs=[pl.BlockSpec(memory_space=pl.ANY)] * 6,
        out_specs=tuple([pl.BlockSpec(memory_space=pltpu.VMEM)] * 5),
        scratch_shapes=[
            pltpu.VMEM(wide, BF16), pltpu.VMEM(wide, BF16), pltpu.VMEM(wide, BF16), pltpu.VMEM(wide, BF16),
            pltpu.VMEM((HL, T), jnp.int32), pltpu.VMEM((HL, C, HD), F32),
            pltpu.VMEM((HL, 4 * T, HD), BF16), pltpu.VMEM(wide, F32), pltpu.VMEM(wide, F32),
            pltpu.VMEM(wide, F32), pltpu.VMEM(wide, F32),
            pltpu.VMEM((ROWS, ROWS), BF16), pltpu.VMEM((ROWS, ROWS), BF16), pltpu.VMEM((HL, ROWS, ROWS), BF16),
            pltpu.VMEM((2, T), F32), pltpu.VMEM((NH, 2, T), F32),
            pltpu.VMEM((2, T), F32), pltpu.VMEM((NH, 2, T), F32),
            pltpu.VMEM((HL, C), BF16), pltpu.VMEM((NX, NZ, HL, C), BF16),
            pltpu.VMEM((8, HD), BF16), pltpu.VMEM((NX, NZ, 8, HD), BF16),
            pltpu.VMEM((2, NS, 16, HD), BF16), pltpu.VMEM((2, NS, 16, HD), BF16),
            pltpu.VMEM((4, NS, 8, HD), BF16), pltpu.VMEM((4, NS, 8, HD), BF16),
            dma((6,)), dma, dma, dma, dma, dma((3,)), dma((3,)), dma, dma, dma, dma,
            dma((2,)), dma((2,)), dma((4,)), dma((4,)),
        ],
        compiler_params=pltpu.CompilerParams(collective_id=0, has_side_effects=True),
    )(query_vectors, key_vectors, value_vectors, upstream, cluster, centroids)
    return pl.pallas_call(
        put_out,
        out_shape=tuple(jax.ShapeDtypeStruct(wide, BF16) for _ in range(4))
        + (jax.ShapeDtypeStruct((HL, C, HD), F32),),
        in_specs=[pl.BlockSpec(memory_space=pltpu.VMEM)] * 5,
        out_specs=tuple([pl.BlockSpec(memory_space=pl.ANY)] * 5),
        scratch_shapes=[dma((5,))],
    )(*(pltpu.with_memory_space_constraint(one, pltpu.VMEM) for one in held))


def solution(mesh):
    placed = (
        P("seq", "head"),
        P("seq", "head"),
        P("seq", "head"),
        P("head", "seq"),
        P("head", None, None),
        P("seq", "head"),
    )
    return jax.shard_map(
        local,
        mesh=mesh,
        in_specs=placed,
        out_specs=(
            P("seq", "head"),
            P("seq", "head"),
            P("seq", "head"),
            P("seq", "head"),
            P("head", None, None),
        ),
        check_vma=False,
    )
```

```python
import functools

import jax
import jax.numpy as jnp
from jax import lax
from jax.experimental import pallas as pl
from jax.experimental.pallas import tpu as pltpu
from jax.sharding import PartitionSpec as P

MASKED = -1e30
EPSILON = 1e-06
RETAIN = 0.9
MESH = pl.DeviceIdType.MESH
F32 = jnp.float32
BF16 = jnp.bfloat16

HD = 128
NS = 64
NX, NZ = 4, 16
NH = 8
HL = 4
T = 128
C = 128
WIDTH = 4096
NEAR = 4
LATER = 11
ROWS = NS * 8


def iota(shape, dim):
    return lax.broadcasted_iota(jnp.int32, shape, dim)


def nt(a, b):
    return lax.dot_general(a, b, (((1,), (1,)), ((), ())), preferred_element_type=F32)


def tn(a, b):
    return lax.dot_general(a, b, (((0,), (0,)), ((), ())), preferred_element_type=F32)


def nn(a, b):
    return lax.dot_general(a, b, (((1,), (0,)), ((), ())), preferred_element_type=F32)


def to_row(column, eye):
    return jnp.sum(eye * column, axis=0, keepdims=True)


def to_col(row, eye):
    return jnp.sum(eye * row, axis=1, keepdims=True)


def kernel(
    q_hbm, k_hbm, v_hbm, u_hbm, cl_hbm, cen_hbm,
    att_o, gq_o, gk_o, gv_o, cen_o,
    q_s, k_s, v_s, u_s, cl_s, cen_s,
    xs, qn_s, kn_s, gql_s, gkl_s, perm, permt, oht,
    sq_send, sq_recv, in_send, in_recv, cnt_send, cnt_recv, cen_send, cen_recv,
    f_send, f_recv, w_send, w_recv,
    load_sem, sq_ss, sq_rs, in_ss, in_rs, cnt_ss, cnt_rs, cen_ss, cen_rs, cex_ss, cex_rs,
    f_ss, f_rs, w_ss, w_rs,
):
    me = lax.axis_index("seq")
    hme = lax.axis_index("head")
    my_x, my_z = me // NZ, me % NZ
    row_of = [((my_x + NX - 1 - e) % NX) * NZ for e in range(NX)]

    def each_peer(act, begin=0, end=NZ):
        def step(j, carry):
            far = NZ // 2 - (j + 1) // 2
            z = (my_z + far * (2 * (j % 2) - 1) + NZ) % NZ
            for e in range(NX):
                act(row_of[e] + z)
            return carry

        lax.fori_loop(begin, min(end, NZ - 1), step, 0)
        if end == NZ:
            for e in range(NX - 1):
                act(row_of[e] + my_z)

    def each_head(act):
        def step(i, carry):
            act((hme + 1 + i) % NH)
            return carry

        lax.fori_loop(0, NH - 1, step, 0)

    barrier = pltpu.get_barrier_semaphore()

    def greet(to):
        pl.semaphore_signal(barrier, 1, device_id=to, device_id_type=MESH)

    for d in range(NEAR, 0, -1):
        for side in (d, NZ - d):
            greet((hme, my_x * NZ + (my_z + side) % NZ))
    for e in range(NX - 1):
        greet((hme, row_of[e] + my_z))
    each_head(lambda p: greet((p, me)))

    loads = [
        pltpu.make_async_copy(src, dst, load_sem.at[n])
        for n, (src, dst) in enumerate(
            ((cl_hbm, cl_s), (q_hbm, q_s), (k_hbm, k_s), (v_hbm, v_s), (u_hbm, u_s), (cen_hbm, cen_s))
        )
    ]
    for load in loads:
        load.start()

    def send(src, dst, ss, rs, to):
        pltpu.make_async_remote_copy(
            src_ref=src, dst_ref=dst, send_sem=ss, recv_sem=rs, device_id=to, device_id_type=MESH
        ).start()

    def send_all(src_at, dst, ss, rs, begin=0, end=NZ):
        each_peer(lambda p: send(src_at(p), dst.at[me], ss, rs, (hme, p)), begin, end)

    def send_heads(src, dst, ss, rs):
        each_head(lambda p: send(src, dst.at[hme], ss, rs, (p, me)))

    def wait_blocks(buf, n, sem):
        part = buf.at[pl.ds(0, n)]
        pltpu.make_async_copy(part, part, sem).wait()

    ic = iota((T, T), 0)
    il = iota((T, T), 1)
    eye = (ic == il).astype(F32)
    before = (ic < il).astype(F32)
    after = (ic > il).astype(F32)

    loads[0].wait()
    member, cnt_col, earlier, cnt_rows = [], [], [], []
    for h in range(HL):
        m = (ic == cl_s[h : h + 1, :]).astype(F32)
        member.append(m)
        mb = m.astype(BF16)
        n = jnp.sum(m, axis=1, keepdims=True)
        cnt_col.append(n)
        cnt_rows.append(to_row(n, eye))
        earlier.append(jnp.sum(tn(mb, mb) * before, axis=0, keepdims=True))
    cnt_own = jnp.concatenate(cnt_rows, axis=0).astype(BF16)
    cnt_send[...] = cnt_own
    cnt_recv[my_x, my_z] = cnt_own

    pl.semaphore_wait(barrier, 2 * NEAR + NX - 1 + NH - 1)
    for d in range(NEAR, 0, -1):
        for side in (d, NZ - d):
            to = (hme, my_x * NZ + (my_z + side) % NZ)
            send(cnt_send, cnt_recv.at[my_x, my_z], cnt_ss.at[0], cnt_rs.at[0], to)

    loads[1].wait()
    loads[2].wait()
    qf = q_s[...].astype(F32)
    q_row = to_row(jnp.sum(qf * qf, axis=1, keepdims=True), eye)
    kf = k_s[...].astype(F32)
    k_row = to_row(jnp.sum(kf * kf, axis=1, keepdims=True), eye)
    sq_own = jnp.concatenate([q_row, k_row], axis=0)
    sq_send[...] = sq_own
    sq_recv[hme] = sq_own
    send_heads(sq_send, sq_recv, sq_ss, sq_rs)

    big_r = iota((ROWS, ROWS), 0)
    big_l = iota((ROWS, ROWS), 1)
    perm[...] = (big_r == ((big_l // 2) % 4) * T + (big_l // 8) * 2 + big_l % 2).astype(F32).astype(BF16)
    permt[...] = (big_l == ((big_r // 2) % 4) * T + (big_r // 8) * 2 + big_r % 2).astype(F32).astype(BF16)

    loads[3].wait()
    loads[4].wait()
    for h in range(HL):
        xs[h, 2 * T : 3 * T, :] = v_s[:, h * HD : (h + 1) * HD]
        xs[h, 3 * T : 4 * T, :] = u_s[:, h * HD : (h + 1) * HD]
    loads[5].wait()

    def normalize():
        wait_blocks(sq_recv, NH - 1, sq_rs)
        squares = jnp.sum(sq_recv[...], axis=0)
        scales = lax.rsqrt(squares * (1.0 / WIDTH) + EPSILON)
        q_scale = to_col(scales[0:1, :], eye)
        k_scale = to_col(scales[1:2, :], eye)
        q_norm = q_s[...].astype(F32) * q_scale
        k_norm = k_s[...].astype(F32) * k_scale
        qn_s[...] = q_norm
        kn_s[...] = k_norm
        q_low = q_norm.astype(BF16)
        k_low = k_norm.astype(BF16)
        for h in range(HL):
            xs[h, 0:T, :] = q_low[:, h * HD : (h + 1) * HD]
            xs[h, T : 2 * T, :] = k_low[:, h * HD : (h + 1) * HD]
        return q_scale, k_scale

    wait_blocks(cnt_recv.at[0], 2 * NEAR, cnt_rs.at[0])
    for side, rows in ((NZ - NEAR, range(NEAR, 0, -1)), (NEAR, range(NZ - NEAR + 1, NZ))):
        to = (hme, my_x * NZ + (my_z + side) % NZ)
        for r in rows:
            part = cnt_recv.at[my_x, (my_z + r) % NZ]
            send(part, part, cnt_ss.at[1], cnt_rs.at[1], to)
    q_scale, k_scale = normalize()
    wait_blocks(cnt_recv.at[0], 2 * NEAR - 1, cnt_rs.at[1])
    for e in range(NX - 1):
        send(cnt_recv.at[my_x], cnt_recv.at[my_x], cnt_ss.at[2], cnt_rs.at[2], (hme, row_of[e] + my_z))
    wait_blocks(cnt_recv, NX - 1, cnt_rs.at[2])
    table = cnt_recv[...].astype(F32).reshape(NS, HL, C)
    table = jnp.concatenate([table, jnp.zeros((NS, 8 - HL, C), F32)], axis=1)
    table = table.reshape(ROWS, C).astype(BF16)
    slot = (iota((T, 1), 0) % 2).astype(F32)
    label_col, label_row, pick_lead, pick_other, renewed_at, place_col = [], [], [], [], [], []
    mine = me.astype(F32)
    for h in range(HL):
        g, half = h // 2, (h % 2) * 8
        spread = (iota((T, ROWS), 1) == (iota((T, ROWS), 0) // 2) * 8 + h).astype(F32).astype(BF16)
        counts = nn(spread, table)
        swing = counts - 1.0
        sb = swing.astype(BF16)
        gram = tn(sb, sb)
        n_row = jnp.sum(swing * swing, axis=0, keepdims=True)
        n_sum = n_row + to_col(n_row, eye)
        opposite = (n_sum + 2.0 * gram == 0.0).astype(F32)
        same = (n_sum - 2.0 * gram == 0.0).astype(F32)
        rank_row = jnp.sum(same * before, axis=0, keepdims=True)
        rank_col = jnp.sum(same * after, axis=1, keepdims=True)
        partner = jnp.where(rank_row == rank_col, opposite, 0.0)
        other_row = jnp.sum(partner * before, axis=0, keepdims=True)
        other_col = jnp.sum(partner * after, axis=1, keepdims=True)
        lead_rank_row = jnp.sum((1.0 - other_col) * before, axis=0, keepdims=True)
        lead_rank_col = jnp.sum((1.0 - other_row) * after, axis=1, keepdims=True)
        partner_rank_col = jnp.sum(partner * lead_rank_row, axis=1, keepdims=True)
        owner_col = jnp.where(other_col > 0.0, partner_rank_col, lead_rank_col)
        base = 8.0 * owner_col + other_col * (2.0 - cnt_col[h])
        place = jnp.sum(member[h] * base, axis=0, keepdims=True) + earlier[h]
        place_col.append(to_col(place, eye))
        target = jnp.concatenate([place + 2.0 * a for a in range(4)], axis=1).astype(jnp.int32)
        onehot = (big_r == target).astype(F32).astype(BF16)
        packed = nn(onehot, xs[h])
        f_send[g, :, half : half + 8, :] = packed.reshape(NS, 8, HD).astype(BF16)
        if half:
            f_recv[g, me] = f_send[g, me]
            send_all(lambda p: f_send.at[g, p], f_recv.at[g], f_ss.at[g], f_rs.at[g])
        lead_mine_row = jnp.where((other_row == 0.0) & (lead_rank_row == mine), 1.0, 0.0)
        lead_count = jnp.sum(counts * lead_mine_row, axis=1, keepdims=True)
        label = (slot < lead_count).astype(F32)
        label_col.append(label)
        label_row.append(to_row(label, eye))
        pick_lead.append(jnp.where((other_col == 0.0) & (owner_col == mine), 1.0, 0.0))
        pick_other.append(jnp.where((other_col > 0.0) & (owner_col == mine), 1.0, 0.0))
        renewed_at.append((owner_col * 8.0 + (2.0 * h) + other_col).astype(jnp.int32))

    for h in range(HL):
        for a in range(4):
            oht[h, a * T : (a + 1) * T, :] = (
                (iota((T, ROWS), 1) == (place_col[h] + 2.0 * a).astype(jnp.int32)).astype(F32).astype(BF16)
            )

    factor = HD ** (-0.5)
    causal = il <= ic

    def attend(h, received):
        rows = nn(perm[...], received)
        k_wide = rows[T : 2 * T]
        u_wide = rows[3 * T : 4 * T]
        low = rows.astype(BF16)
        qr, kr, vr, ur = (low[a * T : (a + 1) * T] for a in range(4))
        allowed = causal & (label_col[h] == label_row[h])
        scores = jnp.where(allowed, nt(qr, kr) * factor, MASKED)
        raised = jnp.exp(scores - jnp.max(scores, axis=1, keepdims=True))
        weights = raised / jnp.sum(raised, axis=1, keepdims=True)
        weights_low = weights.astype(BF16)
        attended = nn(weights_low, vr).astype(BF16)
        row_dot = jnp.sum(u_wide * attended.astype(F32), axis=1, keepdims=True)
        grad_weights = nt(ur, vr)
        grad_scores = (weights * (grad_weights - row_dot) * factor).astype(BF16)
        grad_q = nn(grad_scores, kr).astype(BF16)
        grad_k = tn(grad_scores, qr).astype(BF16)
        grad_v = tn(weights_low, ur).astype(BF16)
        unit = k_wide * lax.rsqrt(jnp.sum(k_wide * k_wide, axis=1, keepdims=True) + EPSILON)
        lead_sum = jnp.sum(unit * label_col[h], axis=0, keepdims=True)
        other_sum = jnp.sum(unit * (1.0 - label_col[h]), axis=0, keepdims=True)
        current = cen_s[h]
        renewed = []
        for chosen, total in ((pick_lead[h], lead_sum), (pick_other[h], other_sum)):
            blended = RETAIN * jnp.sum(current * chosen, axis=0, keepdims=True) + (1.0 - RETAIN) * total
            renewed.append(blended * lax.rsqrt(jnp.sum(blended * blended, axis=1, keepdims=True) + EPSILON))
        return attended, grad_q, grad_k, grad_v, renewed

    def by_device(arrays):
        return nn(permt[...], jnp.concatenate(arrays, axis=0)).reshape(NS, 8, HD).astype(BF16)

    def arrived(part):
        return part.astype(F32).reshape(ROWS, HD).astype(BF16)

    def put_back(n, arrays):
        w_send[n] = by_device(arrays)
        w_recv[n, me] = w_send[n, me]

    def send_back(n, begin=0, end=NZ):
        send_all(lambda p: w_send.at[n, p], w_recv.at[n], w_ss.at[n], w_rs.at[n], begin, end)

    cen_rows = []
    for g in range(2):
        wait_blocks(f_recv.at[g], NS - 1, f_rs.at[g])
        first, second = [], []
        for half in range(2):
            attended, grad_q, grad_k, grad_v, renewed = attend(
                2 * g + half, arrived(f_recv[g, :, half * 8 : half * 8 + 8, :])
            )
            cen_rows += renewed
            first += [grad_q, grad_k]
            second += [attended, grad_v]
        put_back(g, first)
        send_back(g)
        put_back(2 + g, second)
    cen_own = jnp.concatenate(cen_rows, axis=0).astype(BF16)
    cen_send[...] = cen_own
    cen_recv[my_x, my_z] = cen_own

    def cen_along_z(i, carry):
        far = NZ // 2 - (i + 1) // 2
        z = (my_z + far * (2 * (i % 2) - 1) + NZ) % NZ
        send(cen_send, cen_recv.at[my_x, my_z], cen_ss, cen_rs, (hme, my_x * NZ + z))
        return carry

    lax.fori_loop(0, NZ - 1, cen_along_z, 0)
    send_back(2)

    inner_sums = [jnp.zeros((T, 1), F32), jnp.zeros((T, 1), F32)]

    def home_grads(g, received):
        for half in range(2):
            h = 2 * g + half
            cols = slice(h * HD, (h + 1) * HD)
            home = nn(oht[h, half * 2 * T : (half + 1) * 2 * T, :], received)
            gql_s[:, cols] = home[0:T]
            gkl_s[:, cols] = home[T : 2 * T]
            inner_sums[0] += jnp.sum(home[0:T] * qn_s[:, cols], axis=1, keepdims=True)
            inner_sums[1] += jnp.sum(home[T : 2 * T] * kn_s[:, cols], axis=1, keepdims=True)

    def home_values(g, received):
        for half in range(2):
            h = 2 * g + half
            cols = slice(h * HD, (h + 1) * HD)
            home = nn(oht[h, half * 2 * T : (half + 1) * 2 * T, :], received)
            att_o[:, cols] = home[0:T].astype(BF16)
            gv_o[:, cols] = home[T : 2 * T].astype(BF16)

    wait_blocks(w_recv.at[0], NS - 1, w_rs.at[0])
    home_grads(0, arrived(w_recv[0]))
    wait_blocks(w_recv.at[1], NS - 1, w_rs.at[1])
    home_grads(1, arrived(w_recv[1]))
    in_own = jnp.concatenate([to_row(inner_sums[0], eye), to_row(inner_sums[1], eye)], axis=0)
    in_send[...] = in_own
    in_recv[hme] = in_own
    send_heads(in_send, in_recv, in_ss, in_rs)
    send_back(3, 0, LATER)

    wait_blocks(cen_recv.at[my_x], NZ - 1, cen_rs)
    for e in range(NX - 1):
        send(cen_recv.at[my_x], cen_recv.at[my_x], cex_ss, cex_rs, (hme, row_of[e] + my_z))
    send_back(3, LATER, NZ)
    wait_blocks(w_recv.at[2], NS - 1, w_rs.at[2])
    home_values(0, arrived(w_recv[2]))

    wait_blocks(cen_recv, NX - 1, cex_rs)
    renewed = cen_recv[...].astype(F32).reshape(ROWS, HD).astype(BF16)
    for h in range(HL):
        gather = (iota((C, ROWS), 1) == renewed_at[h]).astype(F32).astype(BF16)
        cen_o[h] = nn(gather, renewed)

    wait_blocks(in_recv, NH - 1, in_rs)
    inner = jnp.sum(in_recv[...], axis=0) * (1.0 / WIDTH)
    q_in = to_col(inner[0:1, :], eye)
    k_in = to_col(inner[1:2, :], eye)
    gq_o[...] = (q_scale * (gql_s[...] - qn_s[...] * q_in)).astype(BF16)
    gk_o[...] = (k_scale * (gkl_s[...] - kn_s[...] * k_in)).astype(BF16)

    wait_blocks(sq_recv, NH - 1, sq_ss)
    wait_blocks(in_recv, NH - 1, in_ss)
    wait_blocks(cnt_recv.at[0], 2 * NEAR, cnt_ss.at[0])
    wait_blocks(cnt_recv.at[0], 2 * NEAR - 1, cnt_ss.at[1])
    wait_blocks(cnt_recv, NX - 1, cnt_ss.at[2])
    wait_blocks(cen_recv.at[my_x], NZ - 1, cen_ss)
    wait_blocks(cen_recv, NX - 1, cex_ss)
    for g in range(2):
        wait_blocks(f_send.at[g], NS - 1, f_ss.at[g])

    for n in range(3):
        wait_blocks(w_send.at[n], NS - 1, w_ss.at[n])

    wait_blocks(w_recv.at[3], NS - 1, w_rs.at[3])
    home_values(1, arrived(w_recv[3]))
    wait_blocks(w_send.at[3], NS - 1, w_ss.at[3])


def put_out(*refs):
    n = len(refs) // 2
    sems = refs[-1]
    copies = [pltpu.make_async_copy(refs[i], refs[n + i], sems.at[i]) for i in range(n)]
    for copy in copies:
        copy.start()
    for copy in copies:
        copy.wait()


def local(query_vectors, key_vectors, value_vectors, cluster, centroids, upstream):
    wide = (T, HL * HD)
    dma = pltpu.SemaphoreType.DMA
    held = pl.pallas_call(
        kernel,
        out_shape=tuple(pltpu.VMEM(wide, BF16) for _ in range(4)) + (pltpu.VMEM((HL, C, HD), F32),),
        in_specs=[pl.BlockSpec(memory_space=pl.ANY)] * 6,
        out_specs=tuple([pl.BlockSpec(memory_space=pltpu.VMEM)] * 5),
        scratch_shapes=[
            pltpu.VMEM(wide, BF16), pltpu.VMEM(wide, BF16), pltpu.VMEM(wide, BF16), pltpu.VMEM(wide, BF16),
            pltpu.VMEM((HL, T), jnp.int32), pltpu.VMEM((HL, C, HD), F32),
            pltpu.VMEM((HL, 4 * T, HD), BF16), pltpu.VMEM(wide, F32), pltpu.VMEM(wide, F32),
            pltpu.VMEM(wide, F32), pltpu.VMEM(wide, F32),
            pltpu.VMEM((ROWS, ROWS), BF16), pltpu.VMEM((ROWS, ROWS), BF16), pltpu.VMEM((HL, ROWS, ROWS), BF16),
            pltpu.VMEM((2, T), F32), pltpu.VMEM((NH, 2, T), F32),
            pltpu.VMEM((2, T), F32), pltpu.VMEM((NH, 2, T), F32),
            pltpu.VMEM((HL, C), BF16), pltpu.VMEM((NX, NZ, HL, C), BF16),
            pltpu.VMEM((8, HD), BF16), pltpu.VMEM((NX, NZ, 8, HD), BF16),
            pltpu.VMEM((2, NS, 16, HD), BF16), pltpu.VMEM((2, NS, 16, HD), BF16),
            pltpu.VMEM((4, NS, 8, HD), BF16), pltpu.VMEM((4, NS, 8, HD), BF16),
            dma((6,)), dma, dma, dma, dma, dma((3,)), dma((3,)), dma, dma, dma, dma,
            dma((2,)), dma((2,)), dma((4,)), dma((4,)),
        ],
        compiler_params=pltpu.CompilerParams(collective_id=0, has_side_effects=True),
    )(query_vectors, key_vectors, value_vectors, upstream, cluster, centroids)
    return pl.pallas_call(
        put_out,
        out_shape=tuple(jax.ShapeDtypeStruct(wide, BF16) for _ in range(4))
        + (jax.ShapeDtypeStruct((HL, C, HD), F32),),
        in_specs=[pl.BlockSpec(memory_space=pltpu.VMEM)] * 5,
        out_specs=tuple([pl.BlockSpec(memory_space=pl.ANY)] * 5),
        scratch_shapes=[dma((5,))],
    )(*(pltpu.with_memory_space_constraint(one, pltpu.VMEM) for one in held))


def solution(mesh):
    placed = (
        P("seq", "head"),
        P("seq", "head"),
        P("seq", "head"),
        P("head", "seq"),
        P("head", None, None),
        P("seq", "head"),
    )
    return jax.shard_map(
        local,
        mesh=mesh,
        in_specs=placed,
        out_specs=(
            P("seq", "head"),
            P("seq", "head"),
            P("seq", "head"),
            P("seq", "head"),
            P("head", None, None),
        ),
        check_vma=False,
    )
```

```python
import functools

import jax
import jax.numpy as jnp
from jax import lax
from jax.experimental import pallas as pl
from jax.experimental.pallas import tpu as pltpu
from jax.sharding import PartitionSpec as P

MASKED = -1e30
EPSILON = 1e-06
RETAIN = 0.9
MESH = pl.DeviceIdType.MESH
F32 = jnp.float32
BF16 = jnp.bfloat16

HD = 128
NS = 64
NX, NZ = 4, 16
NH = 8
HL = 4
T = 128
C = 128
WIDTH = 4096
NEAR = 4
HALF = 5
LATER = 11
ROWS = NS * 8


def iota(shape, dim):
    return lax.broadcasted_iota(jnp.int32, shape, dim)


def nt(a, b):
    return lax.dot_general(a, b, (((1,), (1,)), ((), ())), preferred_element_type=F32)


def tn(a, b):
    return lax.dot_general(a, b, (((0,), (0,)), ((), ())), preferred_element_type=F32)


def nn(a, b):
    return lax.dot_general(a, b, (((1,), (0,)), ((), ())), preferred_element_type=F32)


def to_row(column, eye):
    return jnp.sum(eye * column, axis=0, keepdims=True)


def to_col(row, eye):
    return jnp.sum(eye * row, axis=1, keepdims=True)


def kernel(
    q_hbm, k_hbm, v_hbm, u_hbm, cl_hbm, cen_hbm,
    att_o, gq_o, gk_o, gv_o, cen_o,
    q_s, k_s, v_s, u_s, cl_s, cen_s,
    xs, qn_s, kn_s, gql_s, gkl_s, perm, permt, oht,
    sq_send, sq_recv, in_send, in_recv, cnt_send, cnt_recv, cen_send, cen_recv,
    f_send, f_recv, w_send, w_recv,
    load_sem, sq_ss, sq_rs, in_ss, in_rs, cnt_ss, cnt_rs, cen_ss, cen_rs, cex_ss, cex_rs,
    f_ss, f_rs, w_ss, w_rs,
):
    me = lax.axis_index("seq")
    hme = lax.axis_index("head")
    my_x, my_z = me // NZ, me % NZ
    row_of = [((my_x + NX - 1 - e) % NX) * NZ for e in range(NX)]

    def each_peer(act, begin=0, end=NZ):
        def step(j, carry):
            far = NZ // 2 - (j + 1) // 2
            z = (my_z + far * (2 * (j % 2) - 1) + NZ) % NZ
            for e in range(NX):
                act(row_of[e] + z)
            return carry

        lax.fori_loop(begin, min(end, NZ - 1), step, 0)
        if end == NZ:
            for e in range(NX - 1):
                act(row_of[e] + my_z)

    def each_head(act):
        def step(i, carry):
            act((hme + 1 + i) % NH)
            return carry

        lax.fori_loop(0, NH - 1, step, 0)

    barrier = pltpu.get_barrier_semaphore()

    def greet(to):
        pl.semaphore_signal(barrier, 1, device_id=to, device_id_type=MESH)

    for d in range(NEAR, 0, -1):
        for side in (d, NZ - d):
            greet((hme, my_x * NZ + (my_z + side) % NZ))
    for e in range(NX - 1):
        greet((hme, row_of[e] + my_z))
    each_head(lambda p: greet((p, me)))

    loads = [
        pltpu.make_async_copy(src, dst, load_sem.at[n])
        for n, (src, dst) in enumerate(
            ((cl_hbm, cl_s), (q_hbm, q_s), (k_hbm, k_s), (v_hbm, v_s), (u_hbm, u_s), (cen_hbm, cen_s))
        )
    ]
    for load in loads:
        load.start()

    def send(src, dst, ss, rs, to):
        pltpu.make_async_remote_copy(
            src_ref=src, dst_ref=dst, send_sem=ss, recv_sem=rs, device_id=to, device_id_type=MESH
        ).start()

    def send_all(src_at, dst, ss, rs, begin=0, end=NZ):
        each_peer(lambda p: send(src_at(p), dst.at[me], ss, rs, (hme, p)), begin, end)

    def send_heads(src, dst, ss, rs):
        each_head(lambda p: send(src, dst.at[hme], ss, rs, (p, me)))

    def wait_blocks(buf, n, sem):
        part = buf.at[pl.ds(0, n)]
        pltpu.make_async_copy(part, part, sem).wait()

    ic = iota((T, T), 0)
    il = iota((T, T), 1)
    eye = (ic == il).astype(F32)
    before = (ic < il).astype(F32)
    after = (ic > il).astype(F32)

    loads[0].wait()
    member, cnt_col, earlier, cnt_rows = [], [], [], []
    for h in range(HL):
        m = (ic == cl_s[h : h + 1, :]).astype(F32)
        member.append(m)
        mb = m.astype(BF16)
        n = jnp.sum(m, axis=1, keepdims=True)
        cnt_col.append(n)
        cnt_rows.append(to_row(n, eye))
        earlier.append(jnp.sum(tn(mb, mb) * before, axis=0, keepdims=True))
    cnt_own = jnp.concatenate(cnt_rows, axis=0).astype(BF16)
    cnt_send[...] = cnt_own
    cnt_recv[my_x, my_z] = cnt_own

    pl.semaphore_wait(barrier, 2 * NEAR + NX - 1 + NH - 1)
    for d in range(NEAR, 0, -1):
        for side in (d, NZ - d):
            to = (hme, my_x * NZ + (my_z + side) % NZ)
            send(cnt_send, cnt_recv.at[my_x, my_z], cnt_ss.at[0], cnt_rs.at[0], to)

    loads[1].wait()
    loads[2].wait()
    qf = q_s[...].astype(F32)
    q_row = to_row(jnp.sum(qf * qf, axis=1, keepdims=True), eye)
    kf = k_s[...].astype(F32)
    k_row = to_row(jnp.sum(kf * kf, axis=1, keepdims=True), eye)
    sq_own = jnp.concatenate([q_row, k_row], axis=0)
    sq_send[...] = sq_own
    sq_recv[hme] = sq_own
    send_heads(sq_send, sq_recv, sq_ss, sq_rs)

    big_r = iota((ROWS, ROWS), 0)
    big_l = iota((ROWS, ROWS), 1)
    perm[...] = (big_r == ((big_l // 2) % 4) * T + (big_l // 8) * 2 + big_l % 2).astype(F32).astype(BF16)
    permt[...] = (big_l == ((big_r // 2) % 4) * T + (big_r // 8) * 2 + big_r % 2).astype(F32).astype(BF16)

    loads[3].wait()
    loads[4].wait()
    for h in range(HL):
        xs[h, 2 * T : 3 * T, :] = v_s[:, h * HD : (h + 1) * HD]
        xs[h, 3 * T : 4 * T, :] = u_s[:, h * HD : (h + 1) * HD]
    loads[5].wait()

    def normalize():
        wait_blocks(sq_recv, NH - 1, sq_rs)
        squares = jnp.sum(sq_recv[...], axis=0)
        scales = lax.rsqrt(squares * (1.0 / WIDTH) + EPSILON)
        q_scale = to_col(scales[0:1, :], eye)
        k_scale = to_col(scales[1:2, :], eye)
        q_norm = q_s[...].astype(F32) * q_scale
        k_norm = k_s[...].astype(F32) * k_scale
        qn_s[...] = q_norm
        kn_s[...] = k_norm
        q_low = q_norm.astype(BF16)
        k_low = k_norm.astype(BF16)
        for h in range(HL):
            xs[h, 0:T, :] = q_low[:, h * HD : (h + 1) * HD]
            xs[h, T : 2 * T, :] = k_low[:, h * HD : (h + 1) * HD]
        return q_scale, k_scale

    wait_blocks(cnt_recv.at[0], 2 * NEAR, cnt_rs.at[0])
    for side, rows in ((NZ - NEAR, range(NEAR, 0, -1)), (NEAR, range(NZ - NEAR + 1, NZ))):
        to = (hme, my_x * NZ + (my_z + side) % NZ)
        for r in rows:
            part = cnt_recv.at[my_x, (my_z + r) % NZ]
            send(part, part, cnt_ss.at[1], cnt_rs.at[1], to)
    q_scale, k_scale = normalize()
    wait_blocks(cnt_recv.at[0], 2 * NEAR - 1, cnt_rs.at[1])
    for e in range(NX - 1):
        send(cnt_recv.at[my_x], cnt_recv.at[my_x], cnt_ss.at[2], cnt_rs.at[2], (hme, row_of[e] + my_z))
    wait_blocks(cnt_recv, NX - 1, cnt_rs.at[2])
    table = cnt_recv[...].astype(F32).reshape(NS, HL, C)
    table = jnp.concatenate([table, jnp.zeros((NS, 8 - HL, C), F32)], axis=1)
    table = table.reshape(ROWS, C).astype(BF16)
    slot = (iota((T, 1), 0) % 2).astype(F32)
    label_col, label_row, pick_lead, pick_other, renewed_at, place_col = [], [], [], [], [], []
    mine = me.astype(F32)
    for h in range(HL):
        g, half = h // 2, (h % 2) * 8
        spread = (iota((T, ROWS), 1) == (iota((T, ROWS), 0) // 2) * 8 + h).astype(F32).astype(BF16)
        counts = nn(spread, table)
        swing = counts - 1.0
        sb = swing.astype(BF16)
        gram = tn(sb, sb)
        n_row = jnp.sum(swing * swing, axis=0, keepdims=True)
        n_sum = n_row + to_col(n_row, eye)
        opposite = (n_sum + 2.0 * gram == 0.0).astype(F32)
        same = (n_sum - 2.0 * gram == 0.0).astype(F32)
        rank_row = jnp.sum(same * before, axis=0, keepdims=True)
        rank_col = jnp.sum(same * after, axis=1, keepdims=True)
        partner = jnp.where(rank_row == rank_col, opposite, 0.0)
        other_row = jnp.sum(partner * before, axis=0, keepdims=True)
        other_col = jnp.sum(partner * after, axis=1, keepdims=True)
        lead_rank_row = jnp.sum((1.0 - other_col) * before, axis=0, keepdims=True)
        lead_rank_col = jnp.sum((1.0 - other_row) * after, axis=1, keepdims=True)
        partner_rank_col = jnp.sum(partner * lead_rank_row, axis=1, keepdims=True)
        owner_col = jnp.where(other_col > 0.0, partner_rank_col, lead_rank_col)
        base = 8.0 * owner_col + other_col * (2.0 - cnt_col[h])
        place = jnp.sum(member[h] * base, axis=0, keepdims=True) + earlier[h]
        place_col.append(to_col(place, eye))
        target = jnp.concatenate([place + 2.0 * a for a in range(4)], axis=1).astype(jnp.int32)
        onehot = (big_r == target).astype(F32).astype(BF16)
        packed = nn(onehot, xs[h])
        f_send[g, :, half : half + 8, :] = packed.reshape(NS, 8, HD).astype(BF16)
        if half:
            f_recv[g, me] = f_send[g, me]
            send_all(lambda p: f_send.at[g, p], f_recv.at[g], f_ss.at[g], f_rs.at[g])
        lead_mine_row = jnp.where((other_row == 0.0) & (lead_rank_row == mine), 1.0, 0.0)
        lead_count = jnp.sum(counts * lead_mine_row, axis=1, keepdims=True)
        label = (slot < lead_count).astype(F32)
        label_col.append(label)
        label_row.append(to_row(label, eye))
        pick_lead.append(jnp.where((other_col == 0.0) & (owner_col == mine), 1.0, 0.0))
        pick_other.append(jnp.where((other_col > 0.0) & (owner_col == mine), 1.0, 0.0))
        renewed_at.append((owner_col * 8.0 + (2.0 * h) + other_col).astype(jnp.int32))

    for h in range(HL):
        for a in range(4):
            oht[h, a * T : (a + 1) * T, :] = (
                (iota((T, ROWS), 1) == (place_col[h] + 2.0 * a).astype(jnp.int32)).astype(F32).astype(BF16)
            )

    factor = HD ** (-0.5)
    causal = il <= ic

    def attend(h, received):
        rows = nn(perm[...], received)
        k_wide = rows[T : 2 * T]
        u_wide = rows[3 * T : 4 * T]
        low = rows.astype(BF16)
        qr, kr, vr, ur = (low[a * T : (a + 1) * T] for a in range(4))
        allowed = causal & (label_col[h] == label_row[h])
        scores = jnp.where(allowed, nt(qr, kr) * factor, MASKED)
        raised = jnp.exp(scores - jnp.max(scores, axis=1, keepdims=True))
        weights = raised / jnp.sum(raised, axis=1, keepdims=True)
        weights_low = weights.astype(BF16)
        attended = nn(weights_low, vr).astype(BF16)
        row_dot = jnp.sum(u_wide * attended.astype(F32), axis=1, keepdims=True)
        grad_weights = nt(ur, vr)
        grad_scores = (weights * (grad_weights - row_dot) * factor).astype(BF16)
        grad_q = nn(grad_scores, kr).astype(BF16)
        grad_k = tn(grad_scores, qr).astype(BF16)
        grad_v = tn(weights_low, ur).astype(BF16)
        unit = k_wide * lax.rsqrt(jnp.sum(k_wide * k_wide, axis=1, keepdims=True) + EPSILON)
        lead_sum = jnp.sum(unit * label_col[h], axis=0, keepdims=True)
        other_sum = jnp.sum(unit * (1.0 - label_col[h]), axis=0, keepdims=True)
        current = cen_s[h]
        renewed = []
        for chosen, total in ((pick_lead[h], lead_sum), (pick_other[h], other_sum)):
            blended = RETAIN * jnp.sum(current * chosen, axis=0, keepdims=True) + (1.0 - RETAIN) * total
            renewed.append(blended * lax.rsqrt(jnp.sum(blended * blended, axis=1, keepdims=True) + EPSILON))
        return attended, grad_q, grad_k, grad_v, renewed

    def by_device(arrays):
        return nn(permt[...], jnp.concatenate(arrays, axis=0)).reshape(NS, 8, HD).astype(BF16)

    def arrived(part):
        return part.astype(F32).reshape(ROWS, HD).astype(BF16)

    def put_back(n, arrays):
        w_send[n] = by_device(arrays)
        w_recv[n, me] = w_send[n, me]

    def send_back(n, begin=0, end=NZ):
        send_all(lambda p: w_send.at[n, p], w_recv.at[n], w_ss.at[n], w_rs.at[n], begin, end)

    cen_rows = []
    for g in range(2):
        wait_blocks(f_recv.at[g], NS - 1, f_rs.at[g])
        if g == 1:
            send_back(0, HALF, NZ)
        first, second = [], []
        for half in range(2):
            attended, grad_q, grad_k, grad_v, renewed = attend(
                2 * g + half, arrived(f_recv[g, :, half * 8 : half * 8 + 8, :])
            )
            cen_rows += renewed
            first += [grad_q, grad_k]
            second += [attended, grad_v]
        put_back(g, first)
        send_back(g, 0, HALF if g == 0 else NZ)
        put_back(2 + g, second)
    cen_own = jnp.concatenate(cen_rows, axis=0).astype(BF16)
    cen_send[...] = cen_own
    cen_recv[my_x, my_z] = cen_own

    def cen_along_z(i, carry):
        far = NZ // 2 - (i + 1) // 2
        z = (my_z + far * (2 * (i % 2) - 1) + NZ) % NZ
        send(cen_send, cen_recv.at[my_x, my_z], cen_ss, cen_rs, (hme, my_x * NZ + z))
        return carry

    lax.fori_loop(0, NZ - 1, cen_along_z, 0)
    send_back(2)

    inner_sums = [jnp.zeros((T, 1), F32), jnp.zeros((T, 1), F32)]

    def home_grads(g, received):
        for half in range(2):
            h = 2 * g + half
            cols = slice(h * HD, (h + 1) * HD)
            home = nn(oht[h, half * 2 * T : (half + 1) * 2 * T, :], received)
            gql_s[:, cols] = home[0:T]
            gkl_s[:, cols] = home[T : 2 * T]
            inner_sums[0] += jnp.sum(home[0:T] * qn_s[:, cols], axis=1, keepdims=True)
            inner_sums[1] += jnp.sum(home[T : 2 * T] * kn_s[:, cols], axis=1, keepdims=True)

    def home_values(g, received):
        for half in range(2):
            h = 2 * g + half
            cols = slice(h * HD, (h + 1) * HD)
            home = nn(oht[h, half * 2 * T : (half + 1) * 2 * T, :], received)
            att_o[:, cols] = home[0:T].astype(BF16)
            gv_o[:, cols] = home[T : 2 * T].astype(BF16)

    wait_blocks(w_recv.at[0], NS - 1, w_rs.at[0])
    home_grads(0, arrived(w_recv[0]))
    wait_blocks(w_recv.at[1], NS - 1, w_rs.at[1])
    home_grads(1, arrived(w_recv[1]))
    in_own = jnp.concatenate([to_row(inner_sums[0], eye), to_row(inner_sums[1], eye)], axis=0)
    in_send[...] = in_own
    in_recv[hme] = in_own
    send_heads(in_send, in_recv, in_ss, in_rs)
    send_back(3, 0, LATER)

    wait_blocks(cen_recv.at[my_x], NZ - 1, cen_rs)
    for e in range(NX - 1):
        send(cen_recv.at[my_x], cen_recv.at[my_x], cex_ss, cex_rs, (hme, row_of[e] + my_z))
    send_back(3, LATER, NZ)
    wait_blocks(w_recv.at[2], NS - 1, w_rs.at[2])
    home_values(0, arrived(w_recv[2]))

    wait_blocks(cen_recv, NX - 1, cex_rs)
    renewed = cen_recv[...].astype(F32).reshape(ROWS, HD).astype(BF16)
    for h in range(HL):
        gather = (iota((C, ROWS), 1) == renewed_at[h]).astype(F32).astype(BF16)
        cen_o[h] = nn(gather, renewed)

    wait_blocks(in_recv, NH - 1, in_rs)
    inner = jnp.sum(in_recv[...], axis=0) * (1.0 / WIDTH)
    q_in = to_col(inner[0:1, :], eye)
    k_in = to_col(inner[1:2, :], eye)
    gq_o[...] = (q_scale * (gql_s[...] - qn_s[...] * q_in)).astype(BF16)
    gk_o[...] = (k_scale * (gkl_s[...] - kn_s[...] * k_in)).astype(BF16)

    wait_blocks(sq_recv, NH - 1, sq_ss)
    wait_blocks(in_recv, NH - 1, in_ss)
    wait_blocks(cnt_recv.at[0], 2 * NEAR, cnt_ss.at[0])
    wait_blocks(cnt_recv.at[0], 2 * NEAR - 1, cnt_ss.at[1])
    wait_blocks(cnt_recv, NX - 1, cnt_ss.at[2])
    wait_blocks(cen_recv.at[my_x], NZ - 1, cen_ss)
    wait_blocks(cen_recv, NX - 1, cex_ss)
    for g in range(2):
        wait_blocks(f_send.at[g], NS - 1, f_ss.at[g])

    for n in range(3):
        wait_blocks(w_send.at[n], NS - 1, w_ss.at[n])

    wait_blocks(w_recv.at[3], NS - 1, w_rs.at[3])
    home_values(1, arrived(w_recv[3]))
    wait_blocks(w_send.at[3], NS - 1, w_ss.at[3])


def put_out(*refs):
    n = len(refs) // 2
    sems = refs[-1]
    copies = [pltpu.make_async_copy(refs[i], refs[n + i], sems.at[i]) for i in range(n)]
    for copy in copies:
        copy.start()
    for copy in copies:
        copy.wait()


def local(query_vectors, key_vectors, value_vectors, cluster, centroids, upstream):
    wide = (T, HL * HD)
    dma = pltpu.SemaphoreType.DMA
    held = pl.pallas_call(
        kernel,
        out_shape=tuple(pltpu.VMEM(wide, BF16) for _ in range(4)) + (pltpu.VMEM((HL, C, HD), F32),),
        in_specs=[pl.BlockSpec(memory_space=pl.ANY)] * 6,
        out_specs=tuple([pl.BlockSpec(memory_space=pltpu.VMEM)] * 5),
        scratch_shapes=[
            pltpu.VMEM(wide, BF16), pltpu.VMEM(wide, BF16), pltpu.VMEM(wide, BF16), pltpu.VMEM(wide, BF16),
            pltpu.VMEM((HL, T), jnp.int32), pltpu.VMEM((HL, C, HD), F32),
            pltpu.VMEM((HL, 4 * T, HD), BF16), pltpu.VMEM(wide, F32), pltpu.VMEM(wide, F32),
            pltpu.VMEM(wide, F32), pltpu.VMEM(wide, F32),
            pltpu.VMEM((ROWS, ROWS), BF16), pltpu.VMEM((ROWS, ROWS), BF16), pltpu.VMEM((HL, ROWS, ROWS), BF16),
            pltpu.VMEM((2, T), F32), pltpu.VMEM((NH, 2, T), F32),
            pltpu.VMEM((2, T), F32), pltpu.VMEM((NH, 2, T), F32),
            pltpu.VMEM((HL, C), BF16), pltpu.VMEM((NX, NZ, HL, C), BF16),
            pltpu.VMEM((8, HD), BF16), pltpu.VMEM((NX, NZ, 8, HD), BF16),
            pltpu.VMEM((2, NS, 16, HD), BF16), pltpu.VMEM((2, NS, 16, HD), BF16),
            pltpu.VMEM((4, NS, 8, HD), BF16), pltpu.VMEM((4, NS, 8, HD), BF16),
            dma((6,)), dma, dma, dma, dma, dma((3,)), dma((3,)), dma, dma, dma, dma,
            dma((2,)), dma((2,)), dma((4,)), dma((4,)),
        ],
        compiler_params=pltpu.CompilerParams(collective_id=0, has_side_effects=True),
    )(query_vectors, key_vectors, value_vectors, upstream, cluster, centroids)
    return pl.pallas_call(
        put_out,
        out_shape=tuple(jax.ShapeDtypeStruct(wide, BF16) for _ in range(4))
        + (jax.ShapeDtypeStruct((HL, C, HD), F32),),
        in_specs=[pl.BlockSpec(memory_space=pltpu.VMEM)] * 5,
        out_specs=tuple([pl.BlockSpec(memory_space=pl.ANY)] * 5),
        scratch_shapes=[dma((5,))],
    )(*(pltpu.with_memory_space_constraint(one, pltpu.VMEM) for one in held))


def solution(mesh):
    placed = (
        P("seq", "head"),
        P("seq", "head"),
        P("seq", "head"),
        P("head", "seq"),
        P("head", None, None),
        P("seq", "head"),
    )
    return jax.shard_map(
        local,
        mesh=mesh,
        in_specs=placed,
        out_specs=(
            P("seq", "head"),
            P("seq", "head"),
            P("seq", "head"),
            P("seq", "head"),
            P("head", None, None),
        ),
        check_vma=False,
    )
```
